128 devices in a mesh: node: 128 (over y, z, x, core).
Axes of the slice: x: 4, y: 4, z: 4, core: 2. Of those that a mesh axis runs over, the one named last changes fastest.
Arguments:
- node_feats: bfloat16 [131072, 128], P('node'), may hold values from -240 to 240
- weight: bfloat16 [128, 128], replicated, may hold values from -0.5 to 0.5
- att_src: float32 [8, 16], replicated, may hold values from -1.5 to 1.5
- att_dst: float32 [8, 16], replicated, may hold values from -1.5 to 1.5
- out_bias: float32 [128], replicated, may hold values from -3 to 3
- requests: int32 [128, 128], P('node'), may hold values from 0 to 7
- tile_dst: int32 [128, 128], P('node'), may hold values from 0 to 7, as said below
- tile_src: int32 [128, 128], P('node'), may hold values from 0 to 127
- tile_masks: int32 [128, 128, 128, 128], P('node'), may hold values from 0 to 1
- tile_count: int32 [128], P('node'), may hold values from 16 to 128, as said below
Outputs:
- node_out: bfloat16 [131072, 128], P('node')
The draws below stay inside these ranges and needn't reach their ends.
Inputs may be any that keep to these rules, and one draw needn't show every extreme that they name: Within one device the pairs (tile_dst, tile_src) of its 128 slots are distinct. `tile_count`: slots at or past a device's count are unused; some device uses all 128.
All inputs are finite; a program needn't handle non-finite values.
Results may differ from the reference program's by a relative error of at most 0.012.
Values may be sent and summed in bfloat16 or wider, within the bound.
A program may use at most 128 MiB of HBM per device.

```python
import math
import jax
import jax.numpy as jnp
from jax import lax

HEADS = 8
HD = 16
F = 128
BLK = 128
BLK_DEV = 8
TILES = 128
NODES = 131072
N_NODE = 128


def draw_node_feats(key, part):
    key_a = jax.random.fold_in(jax.random.fold_in(key, 5), 0)
    base_draw = jax.random.truncated_normal(key_a, -6.0, 6.0, (NODES, F), jnp.float32)
    return base_draw.astype(jnp.bfloat16)


def tile_pairs(key):
    sub_keys = jax.random.split(jax.random.fold_in(key, 11), N_NODE)
    pairs = jax.vmap(lambda sub_key: jax.random.permutation(sub_key, BLK_DEV * N_NODE)[:TILES])(sub_keys)
    return pairs.astype(jnp.int32)


def draw_tile_dst(key, part):
    return (tile_pairs(key) // N_NODE).astype(jnp.int32)


def draw_tile_src(key, part):
    return (tile_pairs(key) % N_NODE).astype(jnp.int32)


def draw_tile_masks(key, part):
    key_a, key_b = jax.random.split(jax.random.fold_in(key, 23))
    levels = jax.random.randint(key_a, (N_NODE, TILES, 1, 1), 10, 400)
    coins = jax.random.randint(key_b, (N_NODE, TILES, BLK, BLK), 0, 1000)
    return (coins < levels).astype(jnp.int32)


def draw_tile_count(key, part):
    key_a, key_b = jax.random.split(jax.random.fold_in(key, 31))
    levels = jax.random.randint(key_a, (N_NODE,), 0, 4)
    counts = jnp.right_shift(jnp.full((N_NODE,), TILES, jnp.int32), levels)
    busiest = jax.random.randint(key_b, (1,), 0, N_NODE)
    return jnp.where(jnp.arange(N_NODE) == busiest, TILES, counts).astype(jnp.int32)


def place_ends(result, stream_key, least, largest):
    dims = result.shape
    spot = [jax.random.randint(jax.random.fold_in(stream_key, axis), (), 0, dims[axis]) for axis in range(len(dims))]
    result = result.at[tuple(spot)].set(least)
    longest = dims.index(max(dims))
    spot[longest] = (spot[longest] + 1) % dims[longest]
    return result.at[tuple(spot)].set(largest)


def normal_values(rng, dims, width, limit, kind=jnp.bfloat16):
    return jnp.clip(width * jax.random.normal(rng, dims, jnp.float32), -limit, limit).astype(kind)


def setup_inputs(seed: int = 0) -> dict:
    key_of = jax.random.split(jax.random.key(seed), 11)
    return {
        "node_feats": draw_node_feats(jax.random.fold_in(key_of[10], 71), 0),
        "weight": normal_values(key_of[1], (F, F), F ** -0.5, 0.5),
        "att_src": normal_values(key_of[2], (HEADS, HD), HD ** -0.5, 1.5, jnp.float32),
        "att_dst": normal_values(key_of[3], (HEADS, HD), HD ** -0.5, 1.5, jnp.float32),
        "out_bias": normal_values(key_of[4], (F,), 0.5, 3.0, jnp.float32),
        "requests": place_ends(jax.random.randint(key_of[5], (N_NODE, N_NODE), 0, BLK_DEV), jax.random.fold_in(key_of[5], 1), 0, BLK_DEV - 1).astype(jnp.int32),
        "tile_dst": draw_tile_dst(jax.random.fold_in(key_of[10], 71), 0),
        "tile_src": draw_tile_src(jax.random.fold_in(key_of[10], 71), 0),
        "tile_masks": draw_tile_masks(jax.random.fold_in(key_of[10], 71), 0),
        "tile_count": draw_tile_count(jax.random.fold_in(key_of[10], 71), 0),
    }


def leaky_relu(in_value):
    return jnp.where(in_value > 0, in_value, 0.2 * in_value)


def head_scores(projected, att_vec):
    head_count, head_width = att_vec.shape
    wide_heads = projected.astype(jnp.float32).reshape(projected.shape[0], head_count, head_width)
    return jnp.sum(wide_heads * att_vec, axis=-1)


def by_block(scores, block_size):
    row_count, head_count = scores.shape
    return jnp.transpose(scores.reshape(row_count // block_size, block_size, head_count), (0, 2, 1))


def attend_tiles(own_proj, own_src, own_dst, far_proj, far_src, tile_dst, tile_src, tile_mask, live_count, group_size, out_bias):
    num_blocks, block_size, feat_width = own_proj.shape
    head_count = own_src.shape[1]
    head_width = feat_width // head_count
    self_logit = leaky_relu(own_dst + own_src)
    block_ids = jnp.arange(num_blocks, dtype=jnp.int32)
    rounds = (live_count + group_size - 1) // group_size

    def group_terms(step_index):
        first_tile = (step_index * group_size).astype(jnp.int32)
        dst_ids = lax.dynamic_slice_in_dim(tile_dst, first_tile, group_size, 0)
        src_ids = lax.dynamic_slice_in_dim(tile_src, first_tile, group_size, 0)
        edge_mask = lax.dynamic_slice_in_dim(tile_mask, first_tile, group_size, 0)
        is_live = (first_tile + jnp.arange(group_size, dtype=jnp.int32)) < live_count
        dst_term = jnp.take(own_dst, dst_ids, axis=0)
        src_term = jnp.take(far_src, src_ids, axis=0)
        logits = leaky_relu(dst_term[:, :, :, None] + src_term[:, :, None, :])
        kept_edge = ((edge_mask > 0) & is_live[:, None, None])[:, None]
        one_hot = dst_ids[:, None] == block_ids[None, :]
        return dst_ids, src_ids, logits, kept_edge, one_hot

    def max_step(step_index, row_peak):
        dst_ids, src_ids, logits, kept_edge, one_hot = group_terms(step_index)
        tile_max = jnp.max(jnp.where(kept_edge, logits, -jnp.inf), axis=-1)
        candidate = jnp.max(jnp.where(one_hot[:, :, None, None], tile_max[:, None], -jnp.inf), axis=0)
        return jnp.maximum(row_peak, candidate)

    row_peak = lax.fori_loop(0, rounds, max_step, self_logit)
    self_weight = jnp.exp(self_logit - row_peak)
    self_round = lax.optimization_barrier(self_weight.astype(jnp.bfloat16)).astype(jnp.float32)
    own_vals = own_proj.reshape(num_blocks, block_size, head_count, head_width).astype(jnp.float32)
    weighted = jnp.transpose(self_round, (0, 2, 1))[..., None] * own_vals

    def sum_step(step_index, acc_state):
        weighted, norm_sum = acc_state
        dst_ids, src_ids, logits, kept_edge, one_hot = group_terms(step_index)
        row_shift = jnp.take(row_peak, dst_ids, axis=0)
        weights = jnp.exp(jnp.where(kept_edge, logits - row_shift[:, :, :, None], -jnp.inf))
        rounded = weights.astype(jnp.bfloat16).astype(jnp.float32)
        src_vals = jnp.take(far_proj, src_ids, axis=0).reshape(group_size, block_size, head_count, head_width)
        partial_value = jnp.einsum('ghij,gjhd->gihd', rounded, src_vals.astype(jnp.float32))
        pick_mat = one_hot.astype(jnp.float32)
        weighted = weighted + jnp.einsum('gb,gihd->bihd', pick_mat, partial_value, precision=lax.Precision.HIGHEST)
        norm_sum = norm_sum + jnp.einsum('gb,ghi->bhi', pick_mat, jnp.sum(weights, axis=-1), precision=lax.Precision.HIGHEST)
        return weighted, norm_sum

    weighted, norm_sum = lax.fori_loop(0, rounds, sum_step, (weighted, self_weight))
    averaged = weighted / jnp.transpose(norm_sum, (0, 2, 1))[..., None]
    mixed_out = averaged.reshape(num_blocks * block_size, feat_width) + out_bias
    return jax.nn.elu(mixed_out).astype(jnp.bfloat16)


def reference(node_feats, weight, att_src, att_dst, out_bias, requests, tile_dst, tile_src, tile_masks, tile_count):
    projected = jnp.dot(node_feats, weight, preferred_element_type=jnp.float32).astype(jnp.bfloat16)
    proj_blocks = projected.reshape(NODES // BLK, BLK, F)
    src_blocks = by_block(head_scores(projected, att_src), BLK)
    dst_blocks = by_block(head_scores(projected, att_dst), BLK)
    group_size = math.gcd(TILES, 16)
    peer_ids = jnp.arange(N_NODE, dtype=jnp.int32)

    def one_device(device):
        wanted = peer_ids * BLK_DEV + requests[device].astype(jnp.int32)
        far_proj = jnp.take(proj_blocks, wanted, axis=0)
        far_src = jnp.take(src_blocks, wanted, axis=0)
        first_block = (device * BLK_DEV).astype(jnp.int32)
        own_proj = lax.dynamic_slice_in_dim(proj_blocks, first_block, BLK_DEV, 0)
        own_src = lax.dynamic_slice_in_dim(src_blocks, first_block, BLK_DEV, 0)
        own_dst = lax.dynamic_slice_in_dim(dst_blocks, first_block, BLK_DEV, 0)
        return attend_tiles(own_proj, own_src, own_dst, far_proj, far_src, tile_dst[device], tile_src[device], tile_masks[device], tile_count[device], group_size, out_bias)

    results = lax.map(one_device, jnp.arange(N_NODE, dtype=jnp.int32))
    return results.reshape(NODES, F)
```

```python
import functools

import jax
import jax.numpy as jnp
from jax import lax
from jax.experimental import pallas as pl
from jax.experimental.pallas import tpu as pltpu
from jax.sharding import PartitionSpec as P

HEADS = 8
HD = 16
F = 128
BLK = 128
NB = 8
TILES = 128
PEERS = 128
CHUNK = 8
BF = jnp.bfloat16
F32 = jnp.float32
LOW = 40.0
HIGH = 30.0
NT = (((1,), (1,)), ((), ()))


def leaky(v):
    return jnp.maximum(v, 0.2 * v)


def nt_dot(a, b):
    return lax.dot_general(a, b, NT, preferred_element_type=F32)


def split3(a):
    hi = a.astype(BF)
    r1 = a - hi.astype(F32)
    mid = r1.astype(BF)
    lo = (r1 - mid.astype(F32)).astype(BF)
    return hi, mid, lo


def nt_exact(a, b):
    hi, mid, lo = split3(b)
    return (nt_dot(a, lo) + nt_dot(a, mid)) + nt_dot(a, hi)


def iota(shape, dim):
    return lax.broadcasted_iota(jnp.int32, shape, dim)


def attend_kernel(dst_ref, src_ref, cnt_ref, own_ref, far_ref, atts_ref, attd_ref, bias_ref, mask_hbm,
                  out_ref, masks, q_ref, b_ref, d_ref, s_ref, acc, dmat, pmat, slog, sem):
    nchunk = TILES // CHUNK

    def mask_copy(c):
        rows = pl.ds(c * CHUNK, CHUNK)
        return pltpu.make_async_copy(mask_hbm.at[rows], masks.at[rows], sem.at[c])

    def start(c, _):
        mask_copy(c).start()
        return 0

    lax.fori_loop(0, nchunk, start, 0)

    head_of_lane = iota((HEADS, F), 1) // HD
    row_head = iota((HEADS, F), 0)
    own_head = head_of_lane == row_head

    def spread(att):
        return jnp.where(own_head, jnp.concatenate([att] * HEADS, axis=1), 0.0)

    a_s = spread(atts_ref[...])
    a_d = spread(attd_ref[...])
    hi, mid, lo = split3(a_s)
    a24 = jnp.concatenate([hi.astype(F32), mid.astype(F32), lo.astype(F32)], axis=0).astype(BF)

    def score_rows(blocks):
        r = nt_dot(a24, blocks)
        return (r[16:24] + r[8:16]) + r[0:8]

    own_s = score_rows(own_ref[...])
    sig_col = jnp.max(own_s, axis=1, keepdims=True)
    sig_x = jnp.sum(jnp.where(own_head, sig_col, 0.0), axis=0, keepdims=True)

    square_head = iota((F, F), 0) // HD
    same_head = square_head == iota((F, F), 1) // HD
    flat_s = jnp.sum(a_s, axis=0, keepdims=True)
    flat_d = jnp.sum(a_d, axis=0, keepdims=True)
    own = own_ref[...]
    sx = nt_exact(own, jnp.where(same_head, flat_s, 0.0))
    dx = nt_exact(own, jnp.where(same_head, flat_d, 0.0))

    lane = iota((NB * BLK, F), 1)
    first_half = lane < F // 2

    qx = jnp.exp(0.8 * jnp.minimum(dx + sig_x, LOW)).astype(BF)
    for h in range(HEADS):
        pick = (iota((F, F), 0) == h * HD).astype(F32).astype(BF)
        col = jnp.dot(qx, pick, preferred_element_type=F32)
        q_ref[:, h] = col.astype(BF).reshape(NB, BLK, F)

    def init_acc(w):
        vals = own_ref[...].astype(F32)
        turned = pltpu.roll(w, F // 2, 1)
        wv = w * vals
        acc[:, :, 0:F] = jnp.where(first_half, wv, turned).reshape(NB, BLK, F)
        acc[:, :, F:2 * F] = jnp.where(first_half, turned, wv).reshape(NB, BLK, F)

    xo = sx - sig_x
    init_acc(jnp.maximum(qx.astype(F32) * jnp.exp(xo), jnp.exp(0.2 * xo)))

    pair = 2

    def far_scores(i, carry):
        low, high = carry
        p = i * pair
        two = far_ref[pl.ds(p, pair)].reshape(pair * BLK, F)
        raw = score_rows(two)
        s = raw - sig_col
        for k in range(pair):
            part = s[:, k * BLK:(k + 1) * BLK]
            s_ref[p + k] = raw[:, k * BLK:(k + 1) * BLK]
            b_ref[p + k] = jnp.exp(part)
            d_ref[p + k] = jnp.exp(0.2 * part)
            low = jnp.minimum(low, part)
            high = jnp.maximum(high, part)
        return low, high

    zero = jnp.zeros((HEADS, BLK), F32)
    low, high = lax.fori_loop(0, PEERS // pair, far_scores, (zero, zero), unroll=8)
    low = jnp.minimum(low, jnp.min(own_s - sig_col, axis=1, keepdims=True))
    bounded = jnp.logical_and(jnp.min(low) >= -LOW, jnp.max(high) <= HIGH)
    count = cnt_ref[0]

    lane1 = iota((BLK, F), 1)

    def values(src):
        v = far_ref[src]
        sides = []
        for half in range(2):
            parts = []
            for k in range(HEADS // 2):
                h = half * (HEADS // 2) + k
                mine = lane1 // HD == h
                ones = lane1 // HD == (h + HEADS // 2) % HEADS
                parts.append(jnp.where(mine, v, jnp.where(ones, 1.0, 0.0).astype(BF)))
            sides.append(jnp.concatenate(parts, axis=0))
        return sides

    def add_tile(dst, src, weight_of):
        sides = values(src)
        for half in range(2):
            w = jnp.concatenate([weight_of(half * (HEADS // 2) + k) for k in range(HEADS // 2)], axis=1)
            o = jnp.dot(w, sides[half], preferred_element_type=F32)
            acc[dst, :, half * F:(half + 1) * F] += o

    @pl.when(bounded)
    def _():
        def chunk(c, _):
            mask_copy(c).wait()
            live = jnp.clip(count - c * CHUNK, 0, CHUNK)

            def tile(k, _):
                t = c * CHUNK + k
                dst = dst_ref[t]
                src = src_ref[t]
                m = masks[t].astype(F32).astype(BF).reshape(BLK // 16, 16, BLK)

                def weight_of(h):
                    bj = jnp.broadcast_to(b_ref[src, h:h + 1, :], (16, BLK)).astype(BF)
                    dj = jnp.broadcast_to(d_ref[src, h:h + 1, :], (16, BLK)).astype(BF)
                    q = q_ref[dst, h].reshape(BLK // 16, 16, BLK)
                    return (m * jnp.maximum(q * bj[None], dj[None])).reshape(BLK, BLK)

                add_tile(dst, src, weight_of)
                return 0

            lax.fori_loop(0, live, tile, 0)
            return 0

        lax.fori_loop(0, nchunk, chunk, 0)

    @pl.when(jnp.logical_not(bounded))
    def _():
        def finish(c, _):
            mask_copy(c).wait()
            return 0

        lax.fori_loop(0, nchunk, finish, 0)

        for h in range(HEADS):
            dh = jnp.broadcast_to(a_d[h:h + 1], (F, F))
            sh = jnp.broadcast_to(a_s[h:h + 1], (F, F))

            def rows(b, _):
                ob = own_ref[pl.ds(b * BLK, BLK)]
                d = nt_exact(ob, dh)
                dmat[b, h] = d
                pmat[b, h] = leaky(d + nt_exact(ob, sh))
                return 0

            lax.fori_loop(0, NB, rows, 0)

        def expand(b):
            px = pmat[b, 0]
            for h in range(1, HEADS):
                px = jnp.where(lane1 // HD == h, pmat[b, h], px)
            return px

        def keep(b, _):
            slog[pl.ds(b * BLK, BLK)] = expand(b)
            return 0

        lax.fori_loop(0, NB, keep, 0)

        def peak(t, _):
            dst = dst_ref[t]
            src = src_ref[t]
            edge = masks[t] > 0
            for h in range(HEADS):
                lg = leaky(dmat[dst, h] + s_ref[src, h:h + 1, :])
                top = jnp.max(jnp.where(edge, lg, -jnp.inf), axis=1, keepdims=True)
                pmat[dst, h] = jnp.maximum(pmat[dst, h], top)
            return 0

        lax.fori_loop(0, count, peak, 0)

        def settle(b, _):
            rows = pl.ds(b * BLK, BLK)
            slog[rows] = jnp.exp(slog[rows] - expand(b))
            return 0

        lax.fori_loop(0, NB, settle, 0)
        init_acc(slog[...])

        def tile(t, _):
            dst = dst_ref[t]
            src = src_ref[t]
            edge = masks[t] > 0

            def weight_of(h):
                lg = leaky(dmat[dst, h] + s_ref[src, h:h + 1, :])
                return jnp.exp(jnp.where(edge, lg - pmat[dst, h], -jnp.inf)).astype(BF)

            add_tile(dst, src, weight_of)
            return 0

        lax.fori_loop(0, count, tile, 0)

    bias = bias_ref[...]
    for b in range(NB):
        one = acc[b, :, 0:F]
        two = acc[b, :, F:2 * F]
        left = lane1 < F // 2
        top = jnp.where(left, one, two)
        low_part = pltpu.roll(jnp.where(left, two, one), F // 2, 1)
        mixed = top / low_part + bias
        small = mixed * (1.0 + mixed * (0.5 + mixed * (1.0 / 6.0 + mixed * (1.0 / 24.0))))
        neg = jnp.where(mixed > -0.0625, small, jnp.exp(jnp.minimum(mixed, 0.0)) - 1.0)
        out_ref[pl.ds(b * BLK, BLK)] = jnp.where(mixed > 0, mixed, neg).astype(BF)


def attend(own, far, att_src, att_dst, out_bias, dst, src, masks, count):
    vm = pl.BlockSpec(memory_space=pltpu.VMEM)
    sm = pl.BlockSpec(memory_space=pltpu.SMEM)
    return pl.pallas_call(
        attend_kernel,
        out_shape=jax.ShapeDtypeStruct((NB * BLK, F), BF),
        in_specs=[sm, sm, sm, vm, vm, vm, vm, vm, pl.BlockSpec(memory_space=pl.ANY)],
        out_specs=vm,
        scratch_shapes=[
            pltpu.VMEM((TILES, BLK, BLK), jnp.int32),
            pltpu.VMEM((NB, HEADS, BLK, F), BF),
            pltpu.VMEM((PEERS, HEADS, BLK), F32),
            pltpu.VMEM((PEERS, HEADS, BLK), F32),
            pltpu.VMEM((PEERS, HEADS, BLK), F32),
            pltpu.VMEM((NB, BLK, 2 * F), F32),
            pltpu.VMEM((NB, HEADS, BLK, F), F32),
            pltpu.VMEM((NB, HEADS, BLK, F), F32),
            pltpu.VMEM((NB * BLK, F), F32),
            pltpu.SemaphoreType.DMA((TILES // CHUNK,)),
        ],
        compiler_params=pltpu.CompilerParams(vmem_limit_bytes=52 * 1024 * 1024),
        name="attend",
    )(dst, src, count, own, far, att_src, att_dst, out_bias.reshape(1, F), masks)


def local(node_feats, weight, att_src, att_dst, out_bias, requests, tile_dst, tile_src, tile_masks, tile_count):
    projected = jnp.dot(node_feats, weight, preferred_element_type=F32).astype(BF)
    own_proj = projected.reshape(NB, BLK, F)
    wanted = lax.all_to_all(requests, "node", split_axis=1, concat_axis=0, tiled=True).reshape(PEERS)
    far = lax.all_to_all(
        jnp.take(own_proj, wanted, axis=0, mode="clip"), "node", split_axis=0, concat_axis=0, tiled=True
    )
    return attend(projected, far, att_src, att_dst, out_bias, tile_dst[0], tile_src[0], tile_masks[0], tile_count)


def solution(mesh):
    placed = (
        P("node", None), P(), P(), P(), P(), P("node", None), P("node", None), P("node", None),
        P("node", None, None, None), P("node"),
    )
    return jax.shard_map(local, mesh=mesh, in_specs=placed, out_specs=P("node", None), check_vma=False)
```

```python
import functools

import jax
import jax.numpy as jnp
from jax import lax
from jax.experimental import pallas as pl
from jax.experimental.pallas import tpu as pltpu
from jax.sharding import PartitionSpec as P

HEADS = 8
HD = 16
F = 128
BLK = 128
NB = 8
TILES = 128
PEERS = 128
CHUNK = 8
BF = jnp.bfloat16
F32 = jnp.float32
LOW = 40.0
HIGH = 30.0
NT = (((1,), (1,)), ((), ()))


def leaky(v):
    return jnp.maximum(v, 0.2 * v)


def nt_dot(a, b):
    return lax.dot_general(a, b, NT, preferred_element_type=F32)


def split3(a):
    hi = a.astype(BF)
    r1 = a - hi.astype(F32)
    mid = r1.astype(BF)
    lo = (r1 - mid.astype(F32)).astype(BF)
    return hi, mid, lo


def nt_exact(a, b):
    hi, mid, lo = split3(b)
    return (nt_dot(a, lo) + nt_dot(a, mid)) + nt_dot(a, hi)


def iota(shape, dim):
    return lax.broadcasted_iota(jnp.int32, shape, dim)


def attend_kernel(dst_ref, src_ref, cnt_ref, own_ref, far_ref, atts_ref, attd_ref, bias_ref, mask_hbm,
                  out_ref, masks, q_ref, b_ref, d_ref, s_ref, acc, dmat, pmat, slog, sem):
    nchunk = TILES // CHUNK

    def mask_copy(c):
        rows = pl.ds(c * CHUNK, CHUNK)
        return pltpu.make_async_copy(mask_hbm.at[rows], masks.at[rows], sem.at[c])

    def start(c, _):
        mask_copy(c).start()
        return 0

    lax.fori_loop(0, nchunk, start, 0)

    head_of_lane = iota((HEADS, F), 1) // HD
    row_head = iota((HEADS, F), 0)
    own_head = head_of_lane == row_head

    def spread(att):
        return jnp.where(own_head, jnp.concatenate([att] * HEADS, axis=1), 0.0)

    a_s = spread(atts_ref[...])
    a_d = spread(attd_ref[...])
    hi, mid, lo = split3(a_s)
    a24 = jnp.concatenate([hi.astype(F32), mid.astype(F32), lo.astype(F32)], axis=0).astype(BF)

    def score_rows(blocks):
        r = nt_dot(a24, blocks)
        return (r[16:24] + r[8:16]) + r[0:8]

    own_s = score_rows(own_ref[...])
    sig_col = jnp.max(own_s, axis=1, keepdims=True)
    sig_x = jnp.sum(jnp.where(own_head, sig_col, 0.0), axis=0, keepdims=True)

    square_head = iota((F, F), 0) // HD
    same_head = square_head == iota((F, F), 1) // HD
    flat_s = jnp.sum(a_s, axis=0, keepdims=True)
    flat_d = jnp.sum(a_d, axis=0, keepdims=True)
    own = own_ref[...]
    sx = nt_exact(own, jnp.where(same_head, flat_s, 0.0))
    dx = nt_exact(own, jnp.where(same_head, flat_d, 0.0))

    lane = iota((NB * BLK, F), 1)
    first_half = lane < F // 2

    qx = jnp.exp(0.8 * jnp.minimum(dx + sig_x, LOW)).astype(BF)
    for h in range(HEADS):
        pick = (iota((F, F), 0) == h * HD).astype(F32).astype(BF)
        col = jnp.dot(qx, pick, preferred_element_type=F32)
        q_ref[:, h] = col.astype(BF).reshape(NB, BLK, F)

    def init_acc(w):
        vals = own_ref[...].astype(F32)
        turned = pltpu.roll(w, F // 2, 1)
        wv = w * vals
        acc[:, :, 0:F] = jnp.where(first_half, wv, turned).reshape(NB, BLK, F)
        acc[:, :, F:2 * F] = jnp.where(first_half, turned, wv).reshape(NB, BLK, F)

    xo = sx - sig_x
    init_acc(jnp.maximum(qx.astype(F32) * jnp.exp(xo), jnp.exp(0.2 * xo)))

    pair = 2

    def far_scores(i, carry):
        low, high = carry
        p = i * pair
        two = far_ref[pl.ds(p, pair)].reshape(pair * BLK, F)
        raw = score_rows(two)
        s = raw - sig_col
        for k in range(pair):
            part = s[:, k * BLK:(k + 1) * BLK]
            s_ref[p + k] = raw[:, k * BLK:(k + 1) * BLK]
            b_ref[p + k] = jnp.exp(part)
            d_ref[p + k] = jnp.exp(0.2 * part)
            low = jnp.minimum(low, part)
            high = jnp.maximum(high, part)
        return low, high

    zero = jnp.zeros((HEADS, BLK), F32)
    low, high = lax.fori_loop(0, PEERS // pair, far_scores, (zero, zero), unroll=8)
    low = jnp.minimum(low, jnp.min(own_s - sig_col, axis=1, keepdims=True))
    bounded = jnp.logical_and(jnp.min(low) >= -LOW, jnp.max(high) <= HIGH)
    count = cnt_ref[0]

    lane1 = iota((BLK, F), 1)

    def values(src):
        v = far_ref[src]
        sides = []
        for half in range(2):
            parts = []
            for k in range(HEADS // 2):
                h = half * (HEADS // 2) + k
                mine = lane1 // HD == h
                ones = lane1 // HD == (h + HEADS // 2) % HEADS
                parts.append(jnp.where(mine, v, jnp.where(ones, 1.0, 0.0).astype(BF)))
            sides.append(jnp.concatenate(parts, axis=0))
        return sides

    def add_tile(dst, src, weight_of):
        sides = values(src)
        for half in range(2):
            w = jnp.concatenate([weight_of(half * (HEADS // 2) + k) for k in range(HEADS // 2)], axis=1)
            o = jnp.dot(w, sides[half], preferred_element_type=F32)
            acc[dst, :, half * F:(half + 1) * F] += o

    @pl.when(bounded)
    def _():
        def chunk(c, _):
            mask_copy(c).wait()
            live = jnp.clip(count - c * CHUNK, 0, CHUNK)

            def tile(k, _):
                t = c * CHUNK + k
                dst = dst_ref[t]
                src = src_ref[t]
                m = masks[t].astype(F32).astype(BF).reshape(BLK // 16, 16, BLK)

                def weight_of(h):
                    bj = jnp.broadcast_to(b_ref[src, h:h + 1, :], (16, BLK)).astype(BF)
                    dj = jnp.broadcast_to(d_ref[src, h:h + 1, :], (16, BLK)).astype(BF)
                    q = q_ref[dst, h].reshape(BLK // 16, 16, BLK)
                    return (m * jnp.maximum(q * bj[None], dj[None])).reshape(BLK, BLK)

                add_tile(dst, src, weight_of)
                return 0

            lax.fori_loop(0, live, tile, 0)
            return 0

        lax.fori_loop(0, nchunk, chunk, 0)

    @pl.when(jnp.logical_not(bounded))
    def _():
        def finish(c, _):
            mask_copy(c).wait()
            return 0

        lax.fori_loop(0, nchunk, finish, 0)

        for h in range(HEADS):
            dh = jnp.broadcast_to(a_d[h:h + 1], (F, F))
            sh = jnp.broadcast_to(a_s[h:h + 1], (F, F))

            def rows(b, _):
                ob = own_ref[pl.ds(b * BLK, BLK)]
                d = nt_exact(ob, dh)
                dmat[b, h] = d
                pmat[b, h] = leaky(d + nt_exact(ob, sh))
                return 0

            lax.fori_loop(0, NB, rows, 0)

        def expand(b):
            px = pmat[b, 0]
            for h in range(1, HEADS):
                px = jnp.where(lane1 // HD == h, pmat[b, h], px)
            return px

        def keep(b, _):
            slog[pl.ds(b * BLK, BLK)] = expand(b)
            return 0

        lax.fori_loop(0, NB, keep, 0)

        def peak(t, _):
            dst = dst_ref[t]
            src = src_ref[t]
            edge = masks[t] > 0
            for h in range(HEADS):
                lg = leaky(dmat[dst, h] + s_ref[src, h:h + 1, :])
                top = jnp.max(jnp.where(edge, lg, -jnp.inf), axis=1, keepdims=True)
                pmat[dst, h] = jnp.maximum(pmat[dst, h], top)
            return 0

        lax.fori_loop(0, count, peak, 0)

        def settle(b, _):
            rows = pl.ds(b * BLK, BLK)
            slog[rows] = jnp.exp(slog[rows] - expand(b))
            return 0

        lax.fori_loop(0, NB, settle, 0)
        init_acc(slog[...])

        def tile(t, _):
            dst = dst_ref[t]
            src = src_ref[t]
            edge = masks[t] > 0

            def weight_of(h):
                lg = leaky(dmat[dst, h] + s_ref[src, h:h + 1, :])
                return jnp.exp(jnp.where(edge, lg - pmat[dst, h], -jnp.inf)).astype(BF)

            add_tile(dst, src, weight_of)
            return 0

        lax.fori_loop(0, count, tile, 0)

    bias = bias_ref[...]
    for b in range(NB):
        one = acc[b, :, 0:F]
        two = acc[b, :, F:2 * F]
        left = lane1 < F // 2
        top = jnp.where(left, one, two)
        low_part = pltpu.roll(jnp.where(left, two, one), F // 2, 1)
        mixed = top / low_part + bias
        small = mixed * (1.0 + mixed * (0.5 + mixed * (1.0 / 6.0 + mixed * (1.0 / 24.0))))
        neg = jnp.where(mixed > -0.0625, small, jnp.exp(jnp.minimum(mixed, 0.0)) - 1.0)
        out_ref[pl.ds(b * BLK, BLK)] = jnp.where(mixed > 0, mixed, neg).astype(BF)


def attend(own, far, att_src, att_dst, out_bias, dst, src, masks, count):
    vm = pl.BlockSpec(memory_space=pltpu.VMEM)
    sm = pl.BlockSpec(memory_space=pltpu.SMEM)
    return pl.pallas_call(
        attend_kernel,
        out_shape=jax.ShapeDtypeStruct((NB * BLK, F), BF),
        in_specs=[sm, sm, sm, vm, vm, vm, vm, vm, pl.BlockSpec(memory_space=pl.ANY)],
        out_specs=vm,
        scratch_shapes=[
            pltpu.VMEM((TILES, BLK, BLK), jnp.int32),
            pltpu.VMEM((NB, HEADS, BLK, F), BF),
            pltpu.VMEM((PEERS, HEADS, BLK), F32),
            pltpu.VMEM((PEERS, HEADS, BLK), F32),
            pltpu.VMEM((PEERS, HEADS, BLK), F32),
            pltpu.VMEM((NB, BLK, 2 * F), F32),
            pltpu.VMEM((NB, HEADS, BLK, F), F32),
            pltpu.VMEM((NB, HEADS, BLK, F), F32),
            pltpu.VMEM((NB * BLK, F), F32),
            pltpu.SemaphoreType.DMA((TILES // CHUNK,)),
        ],
        compiler_params=pltpu.CompilerParams(vmem_limit_bytes=52 * 1024 * 1024),
        name="attend",
    )(dst, src, count, own, far, att_src, att_dst, out_bias.reshape(1, F), masks)


SIDE = 4
SPLIT = (("z", "y", "x", 0, 48), ("x", "z", "y", 48, 48), ("y", "x", "z", 96, 32))
AXES = ("y", "z", "x")
OTHERS = tuple((off, flip) for off in (1, 3, 2) for flip in (0, 1))
LINE = ((0, 1),) + OTHERS


def peer_list():
    peers = [("x", 0, 1)]
    for axis in AXES:
        for off, flip in OTHERS:
            peers.append((axis, off, flip))
    return peers


PEER_LIST = peer_list()


def peer_slot(axis, off, flip):
    if off == 0:
        return 0
    return PEER_LIST.index((axis, off, flip))


def place(pos, core):
    return ((pos["y"] * SIDE + pos["z"]) * SIDE + pos["x"]) * 2 + core


def exchange_kernel(x_ref, w_ref, req_ref, req_s, far_ref, own_ref, *scratch):
    gathered = tuple(scratch[SIDE * c:SIDE * c + SIDE] for c in range(3))
    picked = scratch[3 * SIDE:3 * SIDE + 3]
    (rq, rqs, ask_s, ask_r, one_s, one_r, two_s, two_r, out_s, out_r, local_sem, smem_sem) = scratch[3 * SIDE + 3:]
    me = lax.axis_index("node")
    core = lax.rem(me, 2)
    pos = {
        "x": lax.rem(lax.div(me, 2), SIDE),
        "z": lax.rem(lax.div(me, 2 * SIDE), SIDE),
        "y": lax.div(me, 2 * SIDE * SIDE),
    }

    def shifted(axis, off):
        return lax.rem(pos[axis] + off, SIDE)

    def device(axis, off, flip):
        where = dict(pos)
        where[axis] = shifted(axis, off)
        return place(where, lax.rem(core + flip, 2))

    def send(src, dst, ssem, rsem, axis, off, flip):
        return pltpu.make_async_remote_copy(
            src_ref=src, dst_ref=dst, send_sem=ssem, recv_sem=rsem,
            device_id=(device(axis, off, flip),), device_id_type=pl.DeviceIdType.MESH,
        )

    barrier = pltpu.get_barrier_semaphore()
    for axis, off, flip in PEER_LIST:
        pl.semaphore_signal(barrier, inc=1, device_id=(device(axis, off, flip),), device_id_type=pl.DeviceIdType.MESH)

    proj = jnp.dot(x_ref[...], w_ref[...], preferred_element_type=F32).astype(BF)
    own_ref[...] = proj
    blocks = proj.reshape(NB, BLK, F)
    for c, (ga, gb, gf, row, rows) in enumerate(SPLIT):
        gathered[c][0][pos[ga]] = blocks[:, row:row + rows]

    pl.semaphore_wait(barrier, len(PEER_LIST))

    def ask(i, back=False):
        axis, off, flip = PEER_LIST[i]
        return send(req_ref, rq.at[i], ask_s.at[i], ask_r.at[i], axis, off, flip)

    steps = (1, 3, 2)

    def first(c, i, back=False):
        ga = SPLIT[c][0]
        off = steps[i]
        mine = gathered[c][0].at[pos[ga]]
        dst = gathered[c][0].at[shifted(ga, SIDE - off)] if back else mine
        return send(mine, dst, one_s.at[c, i], one_r.at[c, i], ga, off, 0)

    turns = (0, 1, 3, 2)

    def second(c, q, i):
        ga, gb = SPLIT[c][:2]
        off = steps[i]
        at = shifted(ga, (SIDE - turns[q]) % SIDE)
        src = gathered[c][0].at[at]
        return send(src, gathered[c][i + 1].at[at], two_s.at[c, q, i], two_r.at[c, q, i], gb, off, 0)

    def landing(c, b_at, f_at, from_core):
        ga, gb, gf, row, rows = SPLIT[c]
        spot = {ga: pl.ds(0, SIDE), gb: b_at, gf: f_at}
        return far_ref.at[spot["y"], spot["z"], spot["x"], from_core, pl.ds(row, rows)]

    def third(c, q, j, back=False):
        ga, gb, gf, row, rows = SPLIT[c]
        off, flip = LINE[j]
        b_at = shifted(gb, (SIDE - turns[q]) % SIDE)
        src = picked[c].at[q, j]
        if back:
            dst = landing(c, b_at, shifted(gf, (SIDE - off) % SIDE), lax.rem(core + flip, 2))
        else:
            dst = landing(c, b_at, pos[gf], core)
        return send(src, dst, out_s.at[c, q, j], out_r.at[c, q, j], gf, off, flip)

    def stay(c, q):
        gb, gf = SPLIT[c][1:3]
        b_at = shifted(gb, (SIDE - turns[q]) % SIDE)
        return pltpu.make_async_copy(picked[c].at[q, len(LINE)], landing(c, b_at, pos[gf], core), local_sem.at[c, q])

    for c in range(3):
        for i in range(3):
            first(c, i).start()
    for i in range(len(PEER_LIST)):
        ask(i).start()
    for i in range(3):
        for c in range(3):
            second(c, 0, i).start()
    for q in range(1, SIDE):
        for c in range(3):
            first(c, q - 1, True).wait_recv()
            for i in range(3):
                second(c, q, i).start()
    for i in range(len(PEER_LIST)):
        ask(i).wait_recv()
    fetch = pltpu.make_async_copy(rq, rqs, smem_sem.at[0])
    fetch.start()
    fetch.wait()

    def pick(c, q):
        ga, gb, gf, row, rows = SPLIT[c]
        b_at = shifted(gb, (SIDE - turns[q]) % SIDE)
        for j in range(len(LINE) + 1):
            for a_at in range(SIDE):
                where = {ga: a_at, gb: b_at, gf: pos[gf]}
                col = place(where, core)
                if j < len(LINE):
                    off, flip = LINE[j]
                    block = rqs[peer_slot(gf, (SIDE - off) % SIDE, flip), 0, col]
                else:
                    block = req_s[0, col]
                picked[c][q, j, a_at] = gathered[c][q][a_at, block]

    for q in range(SIDE):
        for c in range(3):
            if q:
                for k in range(SIDE):
                    second(c, k, q - 1).wait_recv()
            pick(c, q)
            for j in range(len(LINE)):
                third(c, q, j).start()
            stay(c, q).start()

    for q in range(SIDE):
        for c in range(3):
            for j in range(len(LINE)):
                third(c, q, j, True).wait_recv()
            stay(c, q).wait()
    for i in range(len(PEER_LIST)):
        ask(i).wait_send()
    for c in range(3):
        for i in range(3):
            first(c, i).wait_send()
        for q in range(SIDE):
            for i in range(3):
                second(c, q, i).wait_send()
            for j in range(len(LINE)):
                third(c, q, j).wait_send()


def exchange(x, weight, requests):
    vm = pl.BlockSpec(memory_space=pltpu.VMEM)
    dma = pltpu.SemaphoreType.DMA
    peers = len(PEER_LIST)
    lines = len(LINE)
    return pl.pallas_call(
        exchange_kernel,
        out_shape=(
            jax.ShapeDtypeStruct((SIDE, SIDE, SIDE, 2, BLK, F), BF),
            jax.ShapeDtypeStruct((NB * BLK, F), BF),
        ),
        in_specs=[vm, vm, vm, pl.BlockSpec(memory_space=pltpu.SMEM)],
        out_specs=(pl.BlockSpec(memory_space=pl.ANY), vm),
        scratch_shapes=(
            [pltpu.VMEM((SIDE, NB, rows, F), BF) for *_, rows in SPLIT for _ in range(SIDE)]
            + [pltpu.VMEM((SIDE, lines + 1, SIDE, rows, F), BF) for *_, rows in SPLIT]
            + [
                pltpu.VMEM((peers, 1, PEERS), jnp.int32),
                pltpu.SMEM((peers, 1, PEERS), jnp.int32),
                dma((peers,)), dma((peers,)),
                dma((3, 3)), dma((3, 3)),
                dma((3, SIDE, 3)), dma((3, SIDE, 3)),
                dma((3, SIDE, lines)), dma((3, SIDE, lines)),
                dma((3, SIDE)), dma((1,)),
            ]
        ),
        compiler_params=pltpu.CompilerParams(
            collective_id=0, has_side_effects=True, vmem_limit_bytes=32 * 1024 * 1024
        ),
        name="exchange",
    )(x, weight, requests, requests)


def local(node_feats, weight, att_src, att_dst, out_bias, requests, tile_dst, tile_src, tile_masks, tile_count):
    far, own = exchange(node_feats, weight, requests)
    far = far.reshape(PEERS, BLK, F)
    return attend(own, far, att_src, att_dst, out_bias, tile_dst[0], tile_src[0], tile_masks[0], tile_count)


def solution(mesh):
    placed = (
        P("node", None), P(), P(), P(), P(), P("node", None), P("node", None), P("node", None),
        P("node", None, None, None), P("node"),
    )
    return jax.shard_map(local, mesh=mesh, in_specs=placed, out_specs=P("node", None), check_vma=False)
```

```python
import functools

import jax
import jax.numpy as jnp
from jax import lax
from jax.experimental import pallas as pl
from jax.experimental.pallas import tpu as pltpu
from jax.sharding import PartitionSpec as P

HEADS = 8
HD = 16
F = 128
BLK = 128
NB = 8
TILES = 128
PEERS = 128
CHUNK = 8
GROUP = 4
ROWS = 16
BF = jnp.bfloat16
F32 = jnp.float32
LOW = 40.0
HIGH = 30.0
NT = (((1,), (1,)), ((), ()))


def leaky(v):
    return jnp.maximum(v, 0.2 * v)


def nt_dot(a, b):
    return lax.dot_general(a, b, NT, preferred_element_type=F32)


def split3(a):
    hi = a.astype(BF)
    r1 = a - hi.astype(F32)
    mid = r1.astype(BF)
    lo = (r1 - mid.astype(F32)).astype(BF)
    return hi, mid, lo


def nt_exact(a, b):
    hi, mid, lo = split3(b)
    return (nt_dot(a, lo) + nt_dot(a, mid)) + nt_dot(a, hi)


def iota(shape, dim):
    return lax.broadcasted_iota(jnp.int32, shape, dim)


def attend_kernel(dst_ref, src_ref, cnt_ref, own_ref, far_ref, atts_ref, attd_ref, bias_ref, mask_hbm,
                  out_ref, masks, s_ref, acc, dmat, pmat, slog, sem):
    pl.run_scoped(
        functools.partial(attend_body, dst_ref, src_ref, cnt_ref, own_ref, far_ref, atts_ref, attd_ref, bias_ref,
                          mask_hbm, out_ref, masks, s_ref, acc, dmat, pmat, slog, sem),
        pltpu.VMEM((NB, HEADS, BLK, F), BF),
        pltpu.VMEM((PEERS, BLK, F), BF),
        pltpu.VMEM((PEERS, HEADS, ROWS, F), BF),
        pltpu.VMEM((PEERS, HEADS, ROWS, F), BF),
        pltpu.VMEM((GROUP, BLK, BLK), BF),
        pltpu.VMEM((ROWS, F), BF),
    )


def attend_body(dst_ref, src_ref, cnt_ref, own_ref, far_ref, atts_ref, attd_ref, bias_ref, mask_hbm,
                out_ref, masks, s_ref, acc, dmat, pmat, slog, sem, q_ref, v_ref, b_ref, d_ref, m_ref, head_ref):
    nchunk = TILES // CHUNK

    def mask_copy(c):
        rows = pl.ds(c * CHUNK, CHUNK)
        return pltpu.make_async_copy(mask_hbm.at[rows], masks.at[rows], sem.at[c])

    def start(c, _):
        mask_copy(c).start()
        return 0

    lax.fori_loop(0, nchunk, start, 0)

    head_of_lane = iota((HEADS, F), 1) // HD
    row_head = iota((HEADS, F), 0)
    own_head = head_of_lane == row_head

    def spread(att):
        return jnp.where(own_head, jnp.concatenate([att] * HEADS, axis=1), 0.0)

    a_s = spread(atts_ref[...])
    a_d = spread(attd_ref[...])
    hi, mid, lo = split3(a_s)
    a24 = jnp.concatenate([hi.astype(F32), mid.astype(F32), lo.astype(F32)], axis=0).astype(BF)

    def score_rows(blocks):
        r = nt_dot(a24, blocks)
        return (r[16:24] + r[8:16]) + r[0:8]

    own_s = score_rows(own_ref[...])
    sig_col = jnp.max(own_s, axis=1, keepdims=True)
    sig_x = jnp.sum(jnp.where(own_head, sig_col, 0.0), axis=0, keepdims=True)

    square_head = iota((F, F), 0) // HD
    same_head = square_head == iota((F, F), 1) // HD
    flat_s = jnp.sum(a_s, axis=0, keepdims=True)
    flat_d = jnp.sum(a_d, axis=0, keepdims=True)
    own = own_ref[...]
    sx = nt_exact(own, jnp.where(same_head, flat_s, 0.0))
    dx = nt_exact(own, jnp.where(same_head, flat_d, 0.0))

    lane = iota((NB * BLK, F), 1)
    first_half = lane < F // 2

    qx = jnp.exp(0.8 * jnp.minimum(dx + sig_x, LOW)).astype(BF)
    for h in range(HEADS):
        pick = (iota((F, F), 0) == h * HD).astype(F32).astype(BF)
        col = jnp.dot(qx, pick, preferred_element_type=F32)
        q_ref[:, h] = col.astype(BF).reshape(NB, BLK, F)

    def init_acc(w):
        vals = own_ref[...].astype(F32)
        turned = pltpu.roll(w, F // 2, 1)
        wv = w * vals
        acc[:, :, 0:F] = jnp.where(first_half, wv, turned).reshape(NB, BLK, F)
        acc[:, :, F:2 * F] = jnp.where(first_half, turned, wv).reshape(NB, BLK, F)

    xo = sx - sig_x
    init_acc(jnp.maximum(qx.astype(F32) * jnp.exp(xo), jnp.exp(0.2 * xo)))

    pair = 2

    def far_scores(i, carry):
        low, high = carry
        p = i * pair
        two = far_ref[pl.ds(p, pair)].reshape(pair * BLK, F)
        raw = score_rows(two)
        s = raw - sig_col
        for k in range(pair):
            part = s[:, k * BLK:(k + 1) * BLK]
            s_ref[p + k] = raw[:, k * BLK:(k + 1) * BLK]
            bexp = jnp.exp(part)
            dexp = jnp.exp(0.2 * part)
            for h in range(HEADS):
                b_ref[p + k, h] = jnp.broadcast_to(bexp[h:h + 1], (ROWS, BLK)).astype(BF)
                d_ref[p + k, h] = jnp.broadcast_to(dexp[h:h + 1], (ROWS, BLK)).astype(BF)
            v_ref[p + k] = two[k * BLK:(k + 1) * BLK]
            low = jnp.minimum(low, part)
            high = jnp.maximum(high, part)
        return low, high

    zero = jnp.zeros((HEADS, BLK), F32)
    low, high = lax.fori_loop(0, PEERS // pair, far_scores, (zero, zero), unroll=8)
    low = jnp.minimum(low, jnp.min(own_s - sig_col, axis=1, keepdims=True))
    bounded = jnp.logical_and(jnp.min(low) >= -LOW, jnp.max(high) <= HIGH)
    count = cnt_ref[0]

    lane1 = iota((BLK, F), 1)
    head_ref[...] = (iota((ROWS, F), 1) // HD).astype(F32).astype(BF)
    cut = (BLK // ROWS, ROWS, F)

    def values(src):
        v = v_ref[src].reshape(cut)
        head_id = head_ref[...]
        sides = []
        for half in range(2):
            parts = []
            for k in range(HEADS // 2):
                h = half * (HEADS // 2) + k
                mine = jnp.broadcast_to((head_id == h)[None], cut)
                ones = (head_id == (h + HEADS // 2) % HEADS).astype(F32).astype(BF)
                parts.append(jnp.where(mine, v, jnp.broadcast_to(ones[None], cut)).reshape(BLK, F))
            sides.append(jnp.concatenate(parts, axis=0))
        return sides

    def tile_sums(src, weight_of):
        sides = values(src)
        sums = []
        for half in range(2):
            w = jnp.concatenate([weight_of(half * (HEADS // 2) + k) for k in range(HEADS // 2)], axis=1)
            sums.append(jnp.dot(w, sides[half], preferred_element_type=F32))
        return sums

    def add_sums(dst, sums):
        for half in range(2):
            acc[dst, :, half * F:(half + 1) * F] += sums[half]

    @pl.when(bounded)
    def _():
        def chunk(c, _):
            mask_copy(c).wait()
            live = jnp.clip((count - c * CHUNK + GROUP - 1) // GROUP, 0, CHUNK // GROUP)

            def group(g, _):
                todo = []
                for k in range(GROUP):
                    t = c * CHUNK + g * GROUP + k
                    used = (t < count).astype(F32)
                    m_ref[k] = (masks[t].astype(F32) * used).astype(BF)
                for k in range(GROUP):
                    t = c * CHUNK + g * GROUP + k
                    dst = dst_ref[t]
                    src = src_ref[t]
                    m = m_ref[k].reshape(cut)

                    def weight_of(h):
                        q = q_ref[dst, h].reshape(cut)
                        bj = jnp.broadcast_to(b_ref[src, h][None], cut)
                        dj = jnp.broadcast_to(d_ref[src, h][None], cut)
                        return (jnp.maximum(q * bj, dj) * m).reshape(BLK, BLK)

                    todo.append((dst, tile_sums(src, weight_of)))
                for dst, sums in todo:
                    add_sums(dst, sums)
                return 0

            lax.fori_loop(0, live, group, 0)
            return 0

        lax.fori_loop(0, nchunk, chunk, 0)

    @pl.when(jnp.logical_not(bounded))
    def _():
        def finish(c, _):
            mask_copy(c).wait()
            return 0

        lax.fori_loop(0, nchunk, finish, 0)

        for h in range(HEADS):
            dh = jnp.broadcast_to(a_d[h:h + 1], (F, F))
            sh = jnp.broadcast_to(a_s[h:h + 1], (F, F))

            def rows(b, _):
                ob = own_ref[pl.ds(b * BLK, BLK)]
                d = nt_exact(ob, dh)
                dmat[b, h] = d
                pmat[b, h] = leaky(d + nt_exact(ob, sh))
                return 0

            lax.fori_loop(0, NB, rows, 0)

        def expand(b):
            px = pmat[b, 0]
            for h in range(1, HEADS):
                px = jnp.where(lane1 // HD == h, pmat[b, h], px)
            return px

        def keep(b, _):
            slog[pl.ds(b * BLK, BLK)] = expand(b)
            return 0

        lax.fori_loop(0, NB, keep, 0)

        def peak(t, _):
            dst = dst_ref[t]
            src = src_ref[t]
            edge = masks[t] > 0
            for h in range(HEADS):
                lg = leaky(dmat[dst, h] + s_ref[src, h:h + 1, :])
                top = jnp.max(jnp.where(edge, lg, -jnp.inf), axis=1, keepdims=True)
                pmat[dst, h] = jnp.maximum(pmat[dst, h], top)
            return 0

        lax.fori_loop(0, count, peak, 0)

        def settle(b, _):
            rows = pl.ds(b * BLK, BLK)
            slog[rows] = jnp.exp(slog[rows] - expand(b))
            return 0

        lax.fori_loop(0, NB, settle, 0)
        init_acc(slog[...])

        def tile(t, _):
            dst = dst_ref[t]
            src = src_ref[t]
            edge = masks[t] > 0

            def weight_of(h):
                lg = leaky(dmat[dst, h] + s_ref[src, h:h + 1, :])
                return jnp.exp(jnp.where(edge, lg - pmat[dst, h], -jnp.inf)).astype(BF)

            add_sums(dst, tile_sums(src, weight_of))
            return 0

        lax.fori_loop(0, count, tile, 0)

    bias = bias_ref[...]
    for b in range(NB):
        one = acc[b, :, 0:F]
        two = acc[b, :, F:2 * F]
        left = lane1 < F // 2
        top = jnp.where(left, one, two)
        low_part = pltpu.roll(jnp.where(left, two, one), F // 2, 1)
        mixed = top / low_part + bias
        small = mixed * (1.0 + mixed * (0.5 + mixed * (1.0 / 6.0 + mixed * (1.0 / 24.0))))
        neg = jnp.where(mixed > -0.0625, small, jnp.exp(jnp.minimum(mixed, 0.0)) - 1.0)
        out_ref[pl.ds(b * BLK, BLK)] = jnp.where(mixed > 0, mixed, neg).astype(BF)


def attend(own, far, att_src, att_dst, out_bias, dst, src, masks, count):
    vm = pl.BlockSpec(memory_space=pltpu.VMEM)
    sm = pl.BlockSpec(memory_space=pltpu.SMEM)
    return pl.pallas_call(
        attend_kernel,
        out_shape=jax.ShapeDtypeStruct((NB * BLK, F), BF),
        in_specs=[sm, sm, sm, vm, vm, vm, vm, vm, pl.BlockSpec(memory_space=pl.ANY)],
        out_specs=vm,
        scratch_shapes=[
            pltpu.VMEM((TILES, BLK, BLK), jnp.int32),
            pltpu.VMEM((PEERS, HEADS, BLK), F32),
            pltpu.VMEM((NB, BLK, 2 * F), F32),
            pltpu.VMEM((NB, HEADS, BLK, F), F32),
            pltpu.VMEM((NB, HEADS, BLK, F), F32),
            pltpu.VMEM((NB * BLK, F), F32),
            pltpu.SemaphoreType.DMA((TILES // CHUNK,)),
        ],
        compiler_params=pltpu.CompilerParams(vmem_limit_bytes=42 * 1024 * 1024),
        name="attend",
    )(dst, src, count, own, far, att_src, att_dst, out_bias.reshape(1, F), masks)


SIDE = 4
SPLIT = (("z", "y", "x", 0, 48), ("x", "z", "y", 48, 48), ("y", "x", "z", 96, 32))
AXES = ("y", "z", "x")
OTHERS = tuple((off, flip) for off in (1, 3, 2) for flip in (0, 1))
LINE = ((0, 1),) + OTHERS


def peer_list():
    peers = [("x", 0, 1)]
    for axis in AXES:
        for off, flip in OTHERS:
            peers.append((axis, off, flip))
    return peers


PEER_LIST = peer_list()


def peer_slot(axis, off, flip):
    if off == 0:
        return 0
    return PEER_LIST.index((axis, off, flip))


def place(pos, core):
    return ((pos["y"] * SIDE + pos["z"]) * SIDE + pos["x"]) * 2 + core


def exchange_kernel(x_ref, w_ref, req_ref, req_s, far_ref, own_ref, *scratch):
    gathered = tuple(scratch[SIDE * c:SIDE * c + SIDE] for c in range(3))
    picked = scratch[3 * SIDE:3 * SIDE + 3]
    (rq, rqs, ask_s, ask_r, one_s, one_r, two_s, two_r, out_s, out_r, local_sem, smem_sem) = scratch[3 * SIDE + 3:]
    me = lax.axis_index("node")
    core = lax.rem(me, 2)
    pos = {
        "x": lax.rem(lax.div(me, 2), SIDE),
        "z": lax.rem(lax.div(me, 2 * SIDE), SIDE),
        "y": lax.div(me, 2 * SIDE * SIDE),
    }

    def shifted(axis, off):
        return lax.rem(pos[axis] + off, SIDE)

    def device(axis, off, flip):
        where = dict(pos)
        where[axis] = shifted(axis, off)
        return place(where, lax.rem(core + flip, 2))

    def send(src, dst, ssem, rsem, axis, off, flip):
        return pltpu.make_async_remote_copy(
            src_ref=src, dst_ref=dst, send_sem=ssem, recv_sem=rsem,
            device_id=(device(axis, off, flip),), device_id_type=pl.DeviceIdType.MESH,
        )

    barrier = pltpu.get_barrier_semaphore()
    for axis, off, flip in PEER_LIST:
        pl.semaphore_signal(barrier, inc=1, device_id=(device(axis, off, flip),), device_id_type=pl.DeviceIdType.MESH)

    proj = jnp.dot(x_ref[...], w_ref[...], preferred_element_type=F32).astype(BF)
    own_ref[...] = proj
    blocks = proj.reshape(NB, BLK, F)
    for c, (ga, gb, gf, row, rows) in enumerate(SPLIT):
        gathered[c][0][pos[ga]] = blocks[:, row:row + rows]

    pl.semaphore_wait(barrier, len(PEER_LIST))

    def ask(i, back=False):
        axis, off, flip = PEER_LIST[i]
        return send(req_ref, rq.at[i], ask_s.at[i], ask_r.at[i], axis, off, flip)

    steps = (1, 3, 2)

    def first(c, i, back=False):
        ga = SPLIT[c][0]
        off = steps[i]
        mine = gathered[c][0].at[pos[ga]]
        dst = gathered[c][0].at[shifted(ga, SIDE - off)] if back else mine
        return send(mine, dst, one_s.at[c, i], one_r.at[c, i], ga, off, 0)

    turns = (0, 1, 3, 2)

    def second(c, q, i):
        ga, gb = SPLIT[c][:2]
        off = steps[i]
        at = shifted(ga, (SIDE - turns[q]) % SIDE)
        src = gathered[c][0].at[at]
        return send(src, gathered[c][i + 1].at[at], two_s.at[c, q, i], two_r.at[c, q, i], gb, off, 0)

    def landing(c, b_at, f_at, from_core):
        ga, gb, gf, row, rows = SPLIT[c]
        spot = {ga: pl.ds(0, SIDE), gb: b_at, gf: f_at}
        return far_ref.at[spot["y"], spot["z"], spot["x"], from_core, pl.ds(row, rows)]

    def third(c, q, j, back=False):
        ga, gb, gf, row, rows = SPLIT[c]
        off, flip = LINE[j]
        b_at = shifted(gb, (SIDE - turns[q]) % SIDE)
        src = picked[c].at[q, j]
        if back:
            dst = landing(c, b_at, shifted(gf, (SIDE - off) % SIDE), lax.rem(core + flip, 2))
        else:
            dst = landing(c, b_at, pos[gf], core)
        return send(src, dst, out_s.at[c, q, j], out_r.at[c, q, j], gf, off, flip)

    def stay(c, q):
        gb, gf = SPLIT[c][1:3]
        b_at = shifted(gb, (SIDE - turns[q]) % SIDE)
        return pltpu.make_async_copy(picked[c].at[q, len(LINE)], landing(c, b_at, pos[gf], core), local_sem.at[c, q])

    for c in range(3):
        for i in range(3):
            first(c, i).start()
    for i in range(len(PEER_LIST)):
        ask(i).start()
    for i in range(3):
        for c in range(3):
            second(c, 0, i).start()
    for q in range(1, SIDE):
        for c in range(3):
            first(c, q - 1, True).wait_recv()
            for i in range(3):
                second(c, q, i).start()
    for i in range(len(PEER_LIST)):
        ask(i).wait_recv()
    fetch = pltpu.make_async_copy(rq, rqs, smem_sem.at[0])
    fetch.start()
    fetch.wait()

    def pick(c, q):
        ga, gb, gf, row, rows = SPLIT[c]
        b_at = shifted(gb, (SIDE - turns[q]) % SIDE)
        for j in range(len(LINE) + 1):
            for a_at in range(SIDE):
                where = {ga: a_at, gb: b_at, gf: pos[gf]}
                col = place(where, core)
                if j < len(LINE):
                    off, flip = LINE[j]
                    block = rqs[peer_slot(gf, (SIDE - off) % SIDE, flip), 0, col]
                else:
                    block = req_s[0, col]
                picked[c][q, j, a_at] = gathered[c][q][a_at, block]

    for q in range(SIDE):
        for c in range(3):
            if q:
                for k in range(SIDE):
                    second(c, k, q - 1).wait_recv()
            pick(c, q)
            for j in range(len(LINE)):
                third(c, q, j).start()
            stay(c, q).start()

    for q in range(SIDE):
        for c in range(3):
            for j in range(len(LINE)):
                third(c, q, j, True).wait_recv()
            stay(c, q).wait()
    for i in range(len(PEER_LIST)):
        ask(i).wait_send()
    for c in range(3):
        for i in range(3):
            first(c, i).wait_send()
        for q in range(SIDE):
            for i in range(3):
                second(c, q, i).wait_send()
            for j in range(len(LINE)):
                third(c, q, j).wait_send()


def exchange(x, weight, requests):
    vm = pl.BlockSpec(memory_space=pltpu.VMEM)
    dma = pltpu.SemaphoreType.DMA
    peers = len(PEER_LIST)
    lines = len(LINE)
    return pl.pallas_call(
        exchange_kernel,
        out_shape=(
            jax.ShapeDtypeStruct((SIDE, SIDE, SIDE, 2, BLK, F), BF),
            jax.ShapeDtypeStruct((NB * BLK, F), BF),
        ),
        in_specs=[vm, vm, vm, pl.BlockSpec(memory_space=pltpu.SMEM)],
        out_specs=(pl.BlockSpec(memory_space=pl.ANY), vm),
        scratch_shapes=(
            [pltpu.VMEM((SIDE, NB, rows, F), BF) for *_, rows in SPLIT for _ in range(SIDE)]
            + [pltpu.VMEM((SIDE, lines + 1, SIDE, rows, F), BF) for *_, rows in SPLIT]
            + [
                pltpu.VMEM((peers, 1, PEERS), jnp.int32),
                pltpu.SMEM((peers, 1, PEERS), jnp.int32),
                dma((peers,)), dma((peers,)),
                dma((3, 3)), dma((3, 3)),
                dma((3, SIDE, 3)), dma((3, SIDE, 3)),
                dma((3, SIDE, lines)), dma((3, SIDE, lines)),
                dma((3, SIDE)), dma((1,)),
            ]
        ),
        compiler_params=pltpu.CompilerParams(
            collective_id=0, has_side_effects=True, vmem_limit_bytes=32 * 1024 * 1024
        ),
        name="exchange",
    )(x, weight, requests, requests)


def local(node_feats, weight, att_src, att_dst, out_bias, requests, tile_dst, tile_src, tile_masks, tile_count):
    far, own = exchange(node_feats, weight, requests)
    far = far.reshape(PEERS, BLK, F)
    return attend(own, far, att_src, att_dst, out_bias, tile_dst[0], tile_src[0], tile_masks[0], tile_count)


def solution(mesh):
    placed = (
        P("node", None), P(), P(), P(), P(), P("node", None), P("node", None), P("node", None),
        P("node", None, None, None), P("node"),
    )
    return jax.shard_map(local, mesh=mesh, in_specs=placed, out_specs=P("node", None), check_vma=False)
```

```python
import functools

import jax
import jax.numpy as jnp
from jax import lax
from jax.experimental import pallas as pl
from jax.experimental.pallas import tpu as pltpu
from jax.sharding import PartitionSpec as P

HEADS = 8
HD = 16
F = 128
BLK = 128
NB = 8
TILES = 128
PEERS = 128
CHUNK = 8
GROUP = 4
PART = 16
VMEM_ALL = 67043328
ROWS = 16
BF = jnp.bfloat16
F32 = jnp.float32
LOW = 40.0
HIGH = 30.0
NT = (((1,), (1,)), ((), ()))


def leaky(v):
    return jnp.maximum(v, 0.2 * v)


def nt_dot(a, b):
    return lax.dot_general(a, b, NT, preferred_element_type=F32)


def split3(a):
    hi = a.astype(BF)
    r1 = a - hi.astype(F32)
    mid = r1.astype(BF)
    lo = (r1 - mid.astype(F32)).astype(BF)
    return hi, mid, lo


def nt_exact(a, b):
    hi, mid, lo = split3(b)
    return (nt_dot(a, lo) + nt_dot(a, mid)) + nt_dot(a, hi)


def stacked3(a):
    return jnp.concatenate([part.astype(F32) for part in split3(a)], axis=0).astype(BF)


def score_rows(a24, blocks):
    r = nt_dot(a24, blocks)
    return (r[16:24] + r[8:16]) + r[0:8]


def self_sums(acc, own, w):
    first_half = lax.broadcasted_iota(jnp.int32, (NB * BLK, F), 1) < F // 2
    turned = pltpu.roll(w, F // 2, 1)
    wv = w * own.astype(F32)
    acc[:, :, 0:F] = jnp.where(first_half, wv, turned).reshape(NB, BLK, F)
    acc[:, :, F:2 * F] = jnp.where(first_half, turned, wv).reshape(NB, BLK, F)


def iota(shape, dim):
    return lax.broadcasted_iota(jnp.int32, shape, dim)


def attend_kernel(dst_hbm, src_hbm, cnt_hbm, far_hbm, own_hbm, q_hbm, acc_hbm, par_hbm, mask_hbm,
                  out_ref, *scratch):
    pl.run_scoped(
        functools.partial(attend_body, dst_hbm, src_hbm, cnt_hbm, far_hbm, own_hbm, q_hbm, acc_hbm, par_hbm, mask_hbm,
                          out_ref, *scratch),
        pltpu.VMEM((NB, HEADS, BLK, F), BF),
        pltpu.VMEM((PEERS, BLK, F), BF),
        pltpu.VMEM((GROUP, 2, HEADS, ROWS, F), BF),
        pltpu.VMEM((GROUP, BLK, BLK), BF),
        pltpu.VMEM((ROWS, F), BF),
    )


def attend_body(dst_hbm, src_hbm, cnt_hbm, far_hbm, own_hbm, q_hbm, acc_hbm, par_hbm, mask_hbm,
                out_ref, masks, s_ref, bf_ref, df_ref, acc, dmat, pmat, slog, own_ref, par_ref, dst_ref, src_ref, cnt_ref,
                sem, far_sem, in_sem, q_ref, far_ref, bd_ref, m_ref, head_ref):
    nchunk = TILES // CHUNK

    def mask_copy(c):
        rows = pl.ds(c * CHUNK, CHUNK)
        return pltpu.make_async_copy(mask_hbm.at[rows], masks.at[rows], sem.at[c])

    def far_copy(c):
        rows = pl.ds(c * PART, PART)
        return pltpu.make_async_copy(far_hbm.at[rows], far_ref.at[rows], far_sem.at[c])

    inputs = [
        pltpu.make_async_copy(src, dst, in_sem.at[i])
        for i, (src, dst) in enumerate((
            (par_hbm, par_ref), (cnt_hbm, cnt_ref), (dst_hbm, dst_ref), (src_hbm, src_ref),
            (q_hbm, q_ref), (acc_hbm, acc), (own_hbm, own_ref)))
    ]
    inputs[0].start()
    for c in range(PEERS // PART):
        far_copy(c).start()
    for copy in inputs[1:]:
        copy.start()

    def start(c, _):
        mask_copy(c).start()
        return 0

    lax.fori_loop(0, nchunk, start, 0)
    inputs[0].wait()

    a_s = par_ref[0:8]
    a_d = par_ref[8:16]
    sig_col = par_ref[16:24]
    a24 = stacked3(a_s)
    pair = 2

    def far_scores(i, carry):
        low, high = carry
        p = i * pair
        raw = score_rows(a24, far_ref[pl.ds(p, pair)].reshape(pair * BLK, F))
        for k in range(pair):
            mine = raw[:, k * BLK:(k + 1) * BLK]
            part = mine - sig_col
            s_ref[p + k] = mine
            bf_ref[p + k] = jnp.exp(part)
            df_ref[p + k] = jnp.exp(0.2 * part)
            low = jnp.minimum(low, part)
            high = jnp.maximum(high, part)
        return low, high

    zero = jnp.zeros((HEADS, BLK), F32)

    def far_part(c, carry):
        far_copy(c).wait()
        for i in range(PART // pair):
            carry = far_scores(c * (PART // pair) + i, carry)
        return carry

    low, high = lax.fori_loop(0, PEERS // PART, far_part, (zero, zero))
    low = jnp.minimum(low, par_ref[32:40])
    bounded = jnp.logical_and(jnp.min(low) >= -LOW, jnp.max(high) <= HIGH)
    for copy in inputs[1:]:
        copy.wait()
    count = cnt_ref[0, 0]

    lane1 = iota((BLK, F), 1)
    head_ref[...] = (iota((ROWS, F), 1) // HD).astype(F32).astype(BF)
    cut = (BLK // ROWS, ROWS, F)

    def values(v):
        v = v.reshape(cut)
        head_id = head_ref[...]
        sides = []
        for half in range(2):
            parts = []
            for k in range(HEADS // 2):
                h = half * (HEADS // 2) + k
                mine = jnp.broadcast_to((head_id == h)[None], cut)
                ones = (head_id == (h + HEADS // 2) % HEADS).astype(F32).astype(BF)
                parts.append(jnp.where(mine, v, jnp.broadcast_to(ones[None], cut)).reshape(BLK, F))
            sides.append(jnp.concatenate(parts, axis=0))
        return sides

    def tile_sums(v, weight_of):
        sides = values(v)
        sums = []
        for half in range(2):
            w = jnp.concatenate([weight_of(half * (HEADS // 2) + k) for k in range(HEADS // 2)], axis=1)
            sums.append(jnp.dot(w, sides[half], preferred_element_type=F32))
        return sums

    def add_sums(dst, sums):
        for half in range(2):
            acc[dst, :, half * F:(half + 1) * F] += sums[half]

    @pl.when(bounded)
    def _():
        def chunk(c, _):
            mask_copy(c).wait()
            live = jnp.clip((count - c * CHUNK + GROUP - 1) // GROUP, 0, CHUNK // GROUP)

            def group(g, _):
                todo = []
                for k in range(GROUP):
                    t = c * CHUNK + g * GROUP + k
                    src = src_ref[0, t]
                    used = (t < count).astype(F32)
                    m_ref[k] = (masks[t].astype(F32) * used).astype(BF)
                    for h in range(HEADS):
                        bd_ref[k, 0, h] = jnp.broadcast_to(bf_ref[src, h:h + 1, :], (ROWS, BLK)).astype(BF)
                        bd_ref[k, 1, h] = jnp.broadcast_to(df_ref[src, h:h + 1, :], (ROWS, BLK)).astype(BF)
                for k in range(GROUP):
                    t = c * CHUNK + g * GROUP + k
                    dst = dst_ref[0, t]
                    src = src_ref[0, t]
                    m = m_ref[k].reshape(cut)

                    def weight_of(h):
                        q = q_ref[dst, h].reshape(cut)
                        bj = jnp.broadcast_to(bd_ref[k, 0, h][None], cut)
                        dj = jnp.broadcast_to(bd_ref[k, 1, h][None], cut)
                        return (jnp.maximum(q * bj, dj) * m).reshape(BLK, BLK)

                    todo.append((dst, tile_sums(far_ref[src], weight_of)))
                for dst, sums in todo:
                    add_sums(dst, sums)
                return 0

            lax.fori_loop(0, live, group, 0)
            return 0

        lax.fori_loop(0, nchunk, chunk, 0)

    @pl.when(jnp.logical_not(bounded))
    def _():
        def finish(c, _):
            mask_copy(c).wait()
            return 0

        lax.fori_loop(0, nchunk, finish, 0)

        for h in range(HEADS):
            dh = jnp.broadcast_to(a_d[h:h + 1], (F, F))
            sh = jnp.broadcast_to(a_s[h:h + 1], (F, F))

            def rows(b, _):
                ob = own_ref[pl.ds(b * BLK, BLK)]
                d = nt_exact(ob, dh)
                dmat[b, h] = d
                pmat[b, h] = leaky(d + nt_exact(ob, sh))
                return 0

            lax.fori_loop(0, NB, rows, 0)

        def expand(b):
            px = pmat[b, 0]
            for h in range(1, HEADS):
                px = jnp.where(lane1 // HD == h, pmat[b, h], px)
            return px

        def keep(b, _):
            slog[pl.ds(b * BLK, BLK)] = expand(b)
            return 0

        lax.fori_loop(0, NB, keep, 0)

        def peak(t, _):
            dst = dst_ref[0, t]
            src = src_ref[0, t]
            edge = masks[t] > 0
            for h in range(HEADS):
                lg = leaky(dmat[dst, h] + s_ref[src, h:h + 1, :])
                top = jnp.max(jnp.where(edge, lg, -jnp.inf), axis=1, keepdims=True)
                pmat[dst, h] = jnp.maximum(pmat[dst, h], top)
            return 0

        lax.fori_loop(0, count, peak, 0)

        def settle(b, _):
            rows = pl.ds(b * BLK, BLK)
            slog[rows] = jnp.exp(slog[rows] - expand(b))
            return 0

        lax.fori_loop(0, NB, settle, 0)
        self_sums(acc, own_ref[...], slog[...])

        def tile(t, _):
            dst = dst_ref[0, t]
            src = src_ref[0, t]
            edge = masks[t] > 0

            def weight_of(h):
                lg = leaky(dmat[dst, h] + s_ref[src, h:h + 1, :])
                return jnp.exp(jnp.where(edge, lg - pmat[dst, h], -jnp.inf)).astype(BF)

            add_sums(dst, tile_sums(far_ref[src], weight_of))
            return 0

        lax.fori_loop(0, count, tile, 0)

    bias = par_ref[24:25]
    for b in range(NB):
        one = acc[b, :, 0:F]
        two = acc[b, :, F:2 * F]
        left = lane1 < F // 2
        top = jnp.where(left, one, two)
        low_part = pltpu.roll(jnp.where(left, two, one), F // 2, 1)
        mixed = top / low_part + bias
        small = mixed * (1.0 + mixed * (0.5 + mixed * (1.0 / 6.0 + mixed * (1.0 / 24.0))))
        neg = jnp.where(mixed > -0.0625, small, jnp.exp(jnp.minimum(mixed, 0.0)) - 1.0)
        out_ref[pl.ds(b * BLK, BLK)] = jnp.where(mixed > 0, mixed, neg).astype(BF)


def attend(far, own, q, sums, params, dst, src, masks, count):
    vm = pl.BlockSpec(memory_space=pltpu.VMEM)
    hbm = pl.BlockSpec(memory_space=pltpu.HBM)
    return pl.pallas_call(
        attend_kernel,
        out_shape=jax.ShapeDtypeStruct((NB * BLK, F), BF),
        in_specs=[hbm] * 9,
        out_specs=vm,
        scratch_shapes=[
            pltpu.VMEM((TILES, BLK, BLK), jnp.int32),
            pltpu.VMEM((PEERS, HEADS, BLK), F32),
            pltpu.VMEM((PEERS, HEADS, BLK), F32),
            pltpu.VMEM((PEERS, HEADS, BLK), F32),
            pltpu.VMEM((NB, BLK, 2 * F), F32),
            pltpu.VMEM((NB, HEADS, BLK, F), F32),
            pltpu.VMEM((NB, HEADS, BLK, F), F32),
            pltpu.VMEM((NB * BLK, F), F32),
            pltpu.VMEM((NB * BLK, F), BF),
            pltpu.VMEM((40, F), F32),
            pltpu.SMEM((1, TILES), jnp.int32),
            pltpu.SMEM((1, TILES), jnp.int32),
            pltpu.SMEM((1, 1), jnp.int32),
            pltpu.SemaphoreType.DMA((TILES // CHUNK,)),
            pltpu.SemaphoreType.DMA((PEERS // PART,)),
            pltpu.SemaphoreType.DMA((7,)),
        ],
        compiler_params=pltpu.CompilerParams(vmem_limit_bytes=VMEM_ALL),
        name="attend",
    )(dst, src, count.reshape(1, 1), far, own, q, sums, params, masks)


SIDE = 4
SPLIT = (("z", "y", "x"), ("z", "x", "y"), ("y", "x", "z"), ("x", "y", "z"))
WAYS = len(SPLIT)
SPAN = BLK // WAYS
AXES = ("y", "z", "x")
OTHERS = tuple((off, flip) for off in (1, 3, 2) for flip in (0, 1))
LINE = ((0, 1),) + OTHERS
STEPS = (1, 3, 2)
TURNS = (0, 1, 3, 2)


def peer_list():
    peers = [("x", 0, 1)]
    for axis in AXES:
        for off, flip in OTHERS:
            peers.append((axis, off, flip))
    return peers


PEER_LIST = peer_list()


def peer_slot(axis, off, flip):
    if off == 0:
        return 0
    return PEER_LIST.index((axis, off, flip))


def place(pos, core):
    return ((pos["y"] * SIDE + pos["z"]) * SIDE + pos["x"]) * 2 + core


def exchange_kernel(x_hbm, w_hbm, req_hbm, atts_hbm, attd_hbm, bias_hbm,
                    far_ref, own_hbm, q_hbm, acc_hbm, par_hbm, *scratch):
    gathered = tuple(scratch[SIDE * c:SIDE * c + SIDE] for c in range(WAYS))
    picked = scratch[SIDE * WAYS:SIDE * WAYS + WAYS]
    (x_ref, w_ref, req_ref, atts_ref, attd_ref, bias_ref, req_s, rq, rqs, own_ref, q_out, acc_out, par_ref,
     fetch_sem, give_sem,
     ask_s, ask_r, one_s, one_r, two_s, two_r, fwd_s, fwd_r, out_s, out_r, local_sem, smem_sem) = (
        scratch[SIDE * WAYS + WAYS:])
    me = lax.axis_index("node")
    core = lax.rem(me, 2)
    pos = {
        "x": lax.rem(lax.div(me, 2), SIDE),
        "z": lax.rem(lax.div(me, 2 * SIDE), SIDE),
        "y": lax.div(me, 2 * SIDE * SIDE),
    }

    def shifted(axis, off):
        return lax.rem(pos[axis] + off, SIDE)

    def device(axis, off, flip):
        where = dict(pos)
        where[axis] = shifted(axis, off)
        return place(where, lax.rem(core + flip, 2))

    def send(src, dst, ssem, rsem, axis, off, flip):
        return pltpu.make_async_remote_copy(
            src_ref=src, dst_ref=dst, send_sem=ssem, recv_sem=rsem,
            device_id=(device(axis, off, flip),), device_id_type=pl.DeviceIdType.MESH,
        )

    fetches = [
        pltpu.make_async_copy(src, dst, fetch_sem.at[i])
        for i, (src, dst) in enumerate((
            (x_hbm, x_ref), (w_hbm, w_ref), (req_hbm, req_ref), (req_hbm, req_s),
            (atts_hbm, atts_ref), (attd_hbm, attd_ref), (bias_hbm, bias_ref)))
    ]
    for f in fetches:
        f.start()
    barrier = pltpu.get_barrier_semaphore()
    for axis, off, flip in PEER_LIST:
        pl.semaphore_signal(barrier, inc=1, device_id=(device(axis, off, flip),), device_id_type=pl.DeviceIdType.MESH)
    for f in fetches:
        f.wait()

    proj = jnp.dot(x_ref[...], w_ref[...], preferred_element_type=F32).astype(BF)
    own_ref[...] = proj
    blocks = proj.reshape(NB, BLK, F)
    for c, (ga, gb, gf) in enumerate(SPLIT):
        gathered[c][0][pos[ga]] = blocks[:, c * SPAN:(c + 1) * SPAN]

    pl.semaphore_wait(barrier, len(PEER_LIST))

    def ask(i):
        axis, off, flip = PEER_LIST[i]
        return send(req_ref, rq.at[i], ask_s.at[i], ask_r.at[i], axis, off, flip)

    def first(c, i, back=False):
        ga = SPLIT[c][0]
        off = STEPS[i]
        mine = gathered[c][0].at[pos[ga]]
        dst = gathered[c][0].at[shifted(ga, SIDE - off)] if back else mine
        return send(mine, dst, one_s.at[c, i], one_r.at[c, i], ga, off, 0)

    def second(c, k, i):
        ga, gb = SPLIT[c][:2]
        at = shifted(ga, (SIDE - TURNS[k]) % SIDE)
        return send(gathered[c][0].at[at], gathered[c][i + 1].at[at], two_s.at[c, k, i], two_r.at[c, k, i],
                    gb, STEPS[i], 0)

    def onward(c, k, i):
        ga, gb = SPLIT[c][:2]
        at = shifted(ga, (SIDE - TURNS[k]) % SIDE)
        part = pl.ds(i * (NB // 2), NB // 2)
        return send(gathered[c][i + 1].at[at, part], gathered[c][3].at[at, part], fwd_s.at[c, k, i], fwd_r.at[c, k, i],
                    gb, STEPS[i], 0)

    def landing(c, b_at, f_at, from_core):
        ga, gb, gf = SPLIT[c]
        spot = {ga: pl.ds(0, SIDE), gb: b_at, gf: f_at}
        return far_ref.at[spot["y"], spot["z"], spot["x"], from_core, pl.ds(c * SPAN, SPAN)]

    def third(c, q, j, back=False):
        ga, gb, gf = SPLIT[c]
        off, flip = LINE[j]
        b_at = shifted(gb, (SIDE - TURNS[q]) % SIDE)
        if back:
            dst = landing(c, b_at, shifted(gf, (SIDE - off) % SIDE), lax.rem(core + flip, 2))
        else:
            dst = landing(c, b_at, pos[gf], core)
        return send(picked[c].at[q, j], dst, out_s.at[c, q, j], out_r.at[c, q, j], gf, off, flip)

    def stay(c, q):
        gb, gf = SPLIT[c][1:3]
        b_at = shifted(gb, (SIDE - TURNS[q]) % SIDE)
        return pltpu.make_async_copy(picked[c].at[q, len(LINE)], landing(c, b_at, pos[gf], core), local_sem.at[c, q])

    for i in range(3):
        for c in range(WAYS):
            first(c, i).start()
    for i in range(len(PEER_LIST)):
        ask(i).start()
    for i in range(2):
        for c in range(WAYS):
            second(c, 0, i).start()

    own_head = iota((HEADS, F), 1) // HD == iota((HEADS, F), 0)

    def spread(att):
        return jnp.where(own_head, jnp.concatenate([att] * HEADS, axis=1), 0.0)

    a_s = spread(atts_ref[...])
    a_d = spread(attd_ref[...])
    own = own_ref[...]
    own_s = score_rows(stacked3(a_s), own)
    sig_col = jnp.max(own_s, axis=1, keepdims=True)
    sig_x = jnp.sum(jnp.where(own_head, sig_col, 0.0), axis=0, keepdims=True)
    par_ref[0:8] = a_s
    par_ref[8:16] = a_d
    par_ref[16:24] = jnp.broadcast_to(sig_col, (HEADS, F))
    par_ref[24:32] = jnp.broadcast_to(bias_ref[...], (8, F))
    par_ref[32:40] = jnp.broadcast_to(jnp.min(own_s - sig_col, axis=1, keepdims=True), (HEADS, F))

    same_head = iota((F, F), 0) // HD == iota((F, F), 1) // HD
    sx = nt_exact(own, jnp.where(same_head, jnp.sum(a_s, axis=0, keepdims=True), 0.0))
    dx = nt_exact(own, jnp.where(same_head, jnp.sum(a_d, axis=0, keepdims=True), 0.0))
    qx = jnp.exp(0.8 * jnp.minimum(dx + sig_x, LOW)).astype(BF)
    for h in range(HEADS):
        pick_col = (iota((F, F), 0) == h * HD).astype(F32).astype(BF)
        q_out[:, h] = jnp.dot(qx, pick_col, preferred_element_type=F32).astype(BF).reshape(NB, BLK, F)
    xo = sx - sig_x
    self_sums(acc_out, own, jnp.maximum(qx.astype(F32) * jnp.exp(xo), jnp.exp(0.2 * xo)))
    gives = [
        pltpu.make_async_copy(src, dst, give_sem.at[i])
        for i, (src, dst) in enumerate(((own_ref, own_hbm), (q_out, q_hbm), (acc_out, acc_hbm), (par_ref, par_hbm)))
    ]
    for g in gives:
        g.start()

    for k in range(1, SIDE):
        for c in range(WAYS):
            first(c, k - 1, True).wait_recv()
            for i in range(2):
                second(c, k, i).start()
    for i in range(len(PEER_LIST)):
        ask(i).wait_recv()
    fetch = pltpu.make_async_copy(rq, rqs, smem_sem.at[0])
    fetch.start()
    fetch.wait()

    def pick(c, q):
        ga, gb, gf = SPLIT[c]
        b_at = shifted(gb, (SIDE - TURNS[q]) % SIDE)
        for j in range(len(LINE) + 1):
            for a_at in range(SIDE):
                col = place({ga: a_at, gb: b_at, gf: pos[gf]}, core)
                if j < len(LINE):
                    off, flip = LINE[j]
                    block = rqs[peer_slot(gf, (SIDE - off) % SIDE, flip), 0, col]
                else:
                    block = req_s[0, col]
                picked[c][q, j, a_at] = gathered[c][q][a_at, block]

    for q in range(SIDE):
        for c in range(WAYS):
            for k in range(SIDE):
                if q in (1, 2):
                    second(c, k, q - 1).wait_recv()
                    onward(c, k, q - 1).start()
                if q == 3:
                    onward(c, k, 0).wait_recv()
                    onward(c, k, 1).wait_recv()
            pick(c, q)
            for j in range(len(LINE)):
                third(c, q, j).start()
            stay(c, q).start()

    for q in range(SIDE):
        for c in range(WAYS):
            for j in range(len(LINE)):
                third(c, q, j, True).wait_recv()
            stay(c, q).wait()
    for g in gives:
        g.wait()
    for i in range(len(PEER_LIST)):
        ask(i).wait_send()
    for c in range(WAYS):
        for i in range(3):
            first(c, i).wait_send()
        for q in range(SIDE):
            for i in range(2):
                second(c, q, i).wait_send()
                onward(c, q, i).wait_send()
            for j in range(len(LINE)):
                third(c, q, j).wait_send()


def exchange(x, weight, requests, att_src, att_dst, out_bias):
    hbm = pl.BlockSpec(memory_space=pltpu.HBM)
    dma = pltpu.SemaphoreType.DMA
    peers = len(PEER_LIST)
    lines = len(LINE)
    return pl.pallas_call(
        exchange_kernel,
        out_shape=(
            jax.ShapeDtypeStruct((SIDE, SIDE, SIDE, 2, BLK, F), BF),
            jax.ShapeDtypeStruct((NB * BLK, F), BF),
            jax.ShapeDtypeStruct((NB, HEADS, BLK, F), BF),
            jax.ShapeDtypeStruct((NB, BLK, 2 * F), F32),
            jax.ShapeDtypeStruct((40, F), F32),
        ),
        in_specs=[hbm] * 6,
        out_specs=(hbm,) * 5,
        scratch_shapes=(
            [pltpu.VMEM((SIDE, NB, SPAN, F), BF) for _ in range(WAYS * SIDE)]
            + [pltpu.VMEM((SIDE, lines + 1, SIDE, SPAN, F), BF) for _ in range(WAYS)]
            + [
                pltpu.VMEM((NB * BLK, F), BF),
                pltpu.VMEM((F, F), BF),
                pltpu.VMEM((1, PEERS), jnp.int32),
                pltpu.VMEM((HEADS, HD), F32),
                pltpu.VMEM((HEADS, HD), F32),
                pltpu.VMEM((1, F), F32),
                pltpu.SMEM((1, PEERS), jnp.int32),
                pltpu.VMEM((peers, 1, PEERS), jnp.int32),
                pltpu.SMEM((peers, 1, PEERS), jnp.int32),
                pltpu.VMEM((NB * BLK, F), BF),
                pltpu.VMEM((NB, HEADS, BLK, F), BF),
                pltpu.VMEM((NB, BLK, 2 * F), F32),
                pltpu.VMEM((40, F), F32),
                dma((7,)), dma((4,)),
                dma((peers,)), dma((peers,)),
                dma((WAYS, 3)), dma((WAYS, 3)),
                dma((WAYS, SIDE, 2)), dma((WAYS, SIDE, 2)),
                dma((WAYS, SIDE, 2)), dma((WAYS, SIDE, 2)),
                dma((WAYS, SIDE, lines)), dma((WAYS, SIDE, lines)),
                dma((WAYS, SIDE)), dma((1,)),
            ]
        ),
        compiler_params=pltpu.CompilerParams(
            collective_id=0, has_side_effects=True, vmem_limit_bytes=VMEM_ALL
        ),
        name="exchange",
    )(x, weight, requests, att_src, att_dst, out_bias.reshape(1, F))


def local(node_feats, weight, att_src, att_dst, out_bias, requests, tile_dst, tile_src, tile_masks, tile_count):
    far, own, q, sums, params = exchange(node_feats, weight, requests, att_src, att_dst, out_bias)
    far = far.reshape(PEERS, BLK, F)
    return attend(far, own, q, sums, params, tile_dst, tile_src, tile_masks[0], tile_count)


def solution(mesh):
    placed = (
        P("node", None), P(), P(), P(), P(), P("node", None), P("node", None), P("node", None),
        P("node", None, None, None), P("node"),
    )
    return jax.shard_map(local, mesh=mesh, in_specs=placed, out_specs=P("node", None), check_vma=False)
```

```python
import functools

import jax
import jax.numpy as jnp
from jax import lax
from jax.experimental import pallas as pl
from jax.experimental.pallas import tpu as pltpu
from jax.sharding import PartitionSpec as P

HEADS = 8
HD = 16
F = 128
BLK = 128
NB = 8
TILES = 128
PEERS = 128
CHUNK = 16
GROUP = 16
PART = 16
VMEM_ALL = 67043328
ROWS = 16
BF = jnp.bfloat16
F32 = jnp.float32
LOW = 40.0
HIGH = 30.0
NT = (((1,), (1,)), ((), ()))


def leaky(v):
    return jnp.maximum(v, 0.2 * v)


def nt_dot(a, b):
    return lax.dot_general(a, b, NT, preferred_element_type=F32)


def split3(a):
    hi = a.astype(BF)
    r1 = a - hi.astype(F32)
    mid = r1.astype(BF)
    lo = (r1 - mid.astype(F32)).astype(BF)
    return hi, mid, lo


def nt_exact(a, b):
    hi, mid, lo = split3(b)
    return (nt_dot(a, lo) + nt_dot(a, mid)) + nt_dot(a, hi)


def stacked3(a):
    return jnp.concatenate([part.astype(F32) for part in split3(a)], axis=0).astype(BF)


def score_rows(a24, blocks):
    r = nt_dot(a24, blocks)
    return (r[16:24] + r[8:16]) + r[0:8]


def self_sums(acc, own, w):
    first_half = lax.broadcasted_iota(jnp.int32, (NB * BLK, F), 1) < F // 2
    turned = pltpu.roll(w, F // 2, 1)
    wv = w * own.astype(F32)
    acc[:, :, 0:F] = jnp.where(first_half, wv, turned).reshape(NB, BLK, F)
    acc[:, :, F:2 * F] = jnp.where(first_half, turned, wv).reshape(NB, BLK, F)


def iota(shape, dim):
    return lax.broadcasted_iota(jnp.int32, shape, dim)


def attend_kernel(dst_hbm, src_hbm, cnt_hbm, far_hbm, own_hbm, q_hbm, acc_hbm, par_hbm, mask_hbm,
                  out_ref, *scratch):
    pl.run_scoped(
        functools.partial(attend_body, dst_hbm, src_hbm, cnt_hbm, far_hbm, own_hbm, q_hbm, acc_hbm, par_hbm, mask_hbm,
                          out_ref, *scratch),
        pltpu.VMEM((NB, HEADS, BLK, F), BF),
        pltpu.VMEM((PEERS, BLK, F), BF),
        pltpu.VMEM((GROUP, 2, HEADS, ROWS, F), BF),
        pltpu.VMEM((GROUP, BLK, BLK), BF),
        pltpu.VMEM((ROWS, F), BF),
    )


def attend_body(dst_hbm, src_hbm, cnt_hbm, far_hbm, own_hbm, q_hbm, acc_hbm, par_hbm, mask_hbm,
                out_ref, masks, s_ref, bf_ref, df_ref, acc, dmat, pmat, slog, own_ref, par_ref, dst_ref, src_ref, cnt_ref,
                sem, far_sem, in_sem, q_ref, far_ref, bd_ref, m_ref, head_ref):
    nchunk = TILES // CHUNK

    def mask_copy(c):
        rows = pl.ds(c * CHUNK, CHUNK)
        return pltpu.make_async_copy(mask_hbm.at[rows], masks.at[rows], sem.at[c])

    def far_copy(c):
        rows = pl.ds(c * PART, PART)
        return pltpu.make_async_copy(far_hbm.at[rows], far_ref.at[rows], far_sem.at[c])

    inputs = [
        pltpu.make_async_copy(src, dst, in_sem.at[i])
        for i, (src, dst) in enumerate((
            (par_hbm, par_ref), (cnt_hbm, cnt_ref), (dst_hbm, dst_ref), (src_hbm, src_ref),
            (q_hbm, q_ref), (acc_hbm, acc), (own_hbm, own_ref)))
    ]
    inputs[0].start()
    for c in range(PEERS // PART):
        far_copy(c).start()
    for copy in inputs[1:]:
        copy.start()

    def start(c, _):
        mask_copy(c).start()
        return 0

    lax.fori_loop(0, nchunk, start, 0)
    inputs[0].wait()

    a_s = par_ref[0:8]
    a_d = par_ref[8:16]
    sig_col = par_ref[16:24]
    a24 = stacked3(a_s)
    pair = 2

    def far_scores(i, carry):
        low, high = carry
        p = i * pair
        raw = score_rows(a24, far_ref[pl.ds(p, pair)].reshape(pair * BLK, F))
        for k in range(pair):
            mine = raw[:, k * BLK:(k + 1) * BLK]
            part = mine - sig_col
            s_ref[p + k] = mine
            bf_ref[p + k] = jnp.exp(part)
            df_ref[p + k] = jnp.exp(0.2 * part)
            low = jnp.minimum(low, part)
            high = jnp.maximum(high, part)
        return low, high

    zero = jnp.zeros((HEADS, BLK), F32)

    def far_part(c, carry):
        far_copy(c).wait()
        for i in range(PART // pair):
            carry = far_scores(c * (PART // pair) + i, carry)
        return carry

    low, high = lax.fori_loop(0, PEERS // PART, far_part, (zero, zero))
    low = jnp.minimum(low, par_ref[32:40])
    bounded = jnp.logical_and(jnp.min(low) >= -LOW, jnp.max(high) <= HIGH)
    for copy in inputs[1:]:
        copy.wait()
    count = cnt_ref[0, 0]

    lane1 = iota((BLK, F), 1)
    head_ref[...] = (iota((ROWS, F), 1) // HD).astype(F32).astype(BF)
    cut = (BLK // ROWS, ROWS, F)

    def values(v):
        v = v.reshape(cut)
        head_id = head_ref[...]
        sides = []
        for half in range(2):
            parts = []
            for k in range(HEADS // 2):
                h = half * (HEADS // 2) + k
                mine = jnp.broadcast_to((head_id == h)[None], cut)
                ones = (head_id == (h + HEADS // 2) % HEADS).astype(F32).astype(BF)
                parts.append(jnp.where(mine, v, jnp.broadcast_to(ones[None], cut)).reshape(BLK, F))
            sides.append(jnp.concatenate(parts, axis=0))
        return sides

    def tile_sums(v, weight_of):
        sides = values(v)
        sums = []
        for half in range(2):
            w = jnp.concatenate([weight_of(half * (HEADS // 2) + k) for k in range(HEADS // 2)], axis=1)
            sums.append(jnp.dot(w, sides[half], preferred_element_type=F32))
        return sums

    def add_sums(dst, sums):
        for half in range(2):
            acc[dst, :, half * F:(half + 1) * F] += sums[half]

    @pl.when(bounded)
    def _():
        def chunk(c, _):
            mask_copy(c).wait()
            live = jnp.clip((count - c * CHUNK + GROUP - 1) // GROUP, 0, CHUNK // GROUP)

            def group(g, _):
                todo = []
                for k in range(GROUP):
                    t = c * CHUNK + g * GROUP + k
                    src = src_ref[0, t]
                    used = (t < count).astype(F32)
                    m_ref[k] = (masks[t].astype(F32) * used).astype(BF)
                    for h in range(HEADS):
                        bd_ref[k, 0, h] = jnp.broadcast_to(bf_ref[src, h:h + 1, :], (ROWS, BLK)).astype(BF)
                        bd_ref[k, 1, h] = jnp.broadcast_to(df_ref[src, h:h + 1, :], (ROWS, BLK)).astype(BF)
                for k in range(GROUP):
                    t = c * CHUNK + g * GROUP + k
                    dst = dst_ref[0, t]
                    src = src_ref[0, t]
                    m = m_ref[k].reshape(cut)

                    def weight_of(h):
                        q = q_ref[dst, h].reshape(cut)
                        bj = jnp.broadcast_to(bd_ref[k, 0, h][None], cut)
                        dj = jnp.broadcast_to(bd_ref[k, 1, h][None], cut)
                        return (jnp.maximum(q * bj, dj) * m).reshape(BLK, BLK)

                    todo.append((dst, tile_sums(far_ref[src], weight_of)))
                for dst, sums in todo:
                    add_sums(dst, sums)
                return 0

            lax.fori_loop(0, live, group, 0)
            return 0

        lax.fori_loop(0, nchunk, chunk, 0)

    @pl.when(jnp.logical_not(bounded))
    def _():
        def finish(c, _):
            mask_copy(c).wait()
            return 0

        lax.fori_loop(0, nchunk, finish, 0)

        for h in range(HEADS):
            dh = jnp.broadcast_to(a_d[h:h + 1], (F, F))
            sh = jnp.broadcast_to(a_s[h:h + 1], (F, F))

            def rows(b, _):
                ob = own_ref[pl.ds(b * BLK, BLK)]
                d = nt_exact(ob, dh)
                dmat[b, h] = d
                pmat[b, h] = leaky(d + nt_exact(ob, sh))
                return 0

            lax.fori_loop(0, NB, rows, 0)

        def expand(b):
            px = pmat[b, 0]
            for h in range(1, HEADS):
                px = jnp.where(lane1 // HD == h, pmat[b, h], px)
            return px

        def keep(b, _):
            slog[pl.ds(b * BLK, BLK)] = expand(b)
            return 0

        lax.fori_loop(0, NB, keep, 0)

        def peak(t, _):
            dst = dst_ref[0, t]
            src = src_ref[0, t]
            edge = masks[t] > 0
            for h in range(HEADS):
                lg = leaky(dmat[dst, h] + s_ref[src, h:h + 1, :])
                top = jnp.max(jnp.where(edge, lg, -jnp.inf), axis=1, keepdims=True)
                pmat[dst, h] = jnp.maximum(pmat[dst, h], top)
            return 0

        lax.fori_loop(0, count, peak, 0)

        def settle(b, _):
            rows = pl.ds(b * BLK, BLK)
            slog[rows] = jnp.exp(slog[rows] - expand(b))
            return 0

        lax.fori_loop(0, NB, settle, 0)
        self_sums(acc, own_ref[...], slog[...])

        def tile(t, _):
            dst = dst_ref[0, t]
            src = src_ref[0, t]
            edge = masks[t] > 0

            def weight_of(h):
                lg = leaky(dmat[dst, h] + s_ref[src, h:h + 1, :])
                return jnp.exp(jnp.where(edge, lg - pmat[dst, h], -jnp.inf)).astype(BF)

            add_sums(dst, tile_sums(far_ref[src], weight_of))
            return 0

        lax.fori_loop(0, count, tile, 0)

    bias = par_ref[24:25]
    for b in range(NB):
        one = acc[b, :, 0:F]
        two = acc[b, :, F:2 * F]
        left = lane1 < F // 2
        top = jnp.where(left, one, two)
        low_part = pltpu.roll(jnp.where(left, two, one), F // 2, 1)
        mixed = top / low_part + bias
        small = mixed * (1.0 + mixed * (0.5 + mixed * (1.0 / 6.0 + mixed * (1.0 / 24.0))))
        neg = jnp.where(mixed > -0.0625, small, jnp.exp(jnp.minimum(mixed, 0.0)) - 1.0)
        out_ref[pl.ds(b * BLK, BLK)] = jnp.where(mixed > 0, mixed, neg).astype(BF)


def attend(far, own, q, sums, params, dst, src, masks, count):
    vm = pl.BlockSpec(memory_space=pltpu.VMEM)
    hbm = pl.BlockSpec(memory_space=pltpu.HBM)
    return pl.pallas_call(
        attend_kernel,
        out_shape=jax.ShapeDtypeStruct((NB * BLK, F), BF),
        in_specs=[hbm] * 9,
        out_specs=vm,
        scratch_shapes=[
            pltpu.VMEM((TILES, BLK, BLK), jnp.int32),
            pltpu.VMEM((PEERS, HEADS, BLK), F32),
            pltpu.VMEM((PEERS, HEADS, BLK), F32),
            pltpu.VMEM((PEERS, HEADS, BLK), F32),
            pltpu.VMEM((NB, BLK, 2 * F), F32),
            pltpu.VMEM((NB, HEADS, BLK, F), F32),
            pltpu.VMEM((NB, HEADS, BLK, F), F32),
            pltpu.VMEM((NB * BLK, F), F32),
            pltpu.VMEM((NB * BLK, F), BF),
            pltpu.VMEM((40, F), F32),
            pltpu.SMEM((1, TILES), jnp.int32),
            pltpu.SMEM((1, TILES), jnp.int32),
            pltpu.SMEM((1, 1), jnp.int32),
            pltpu.SemaphoreType.DMA((TILES // CHUNK,)),
            pltpu.SemaphoreType.DMA((PEERS // PART,)),
            pltpu.SemaphoreType.DMA((7,)),
        ],
        compiler_params=pltpu.CompilerParams(vmem_limit_bytes=VMEM_ALL),
        name="attend",
    )(dst, src, count.reshape(1, 1), far, own, q, sums, params, masks)


SIDE = 4
SPLIT = (("z", "y", "x"), ("x", "z", "y"), ("y", "x", "z"))
ROW_AT = (0, 48, 96)
SPANS = (48, 48, 32)
WAYS = len(SPLIT)
AXES = ("y", "z", "x")
OTHERS = tuple((off, flip) for off in (1, 3, 2) for flip in (0, 1))
LINE = ((0, 1),) + OTHERS
STEPS = (1, 3, 2)
TURNS = (0, 1, 3, 2)


def peer_list():
    peers = [("x", 0, 1)]
    for axis in AXES:
        for off, flip in OTHERS:
            peers.append((axis, off, flip))
    return peers


PEER_LIST = peer_list()


def peer_slot(axis, off, flip):
    if off == 0:
        return 0
    return PEER_LIST.index((axis, off, flip))


def place(pos, core):
    return ((pos["y"] * SIDE + pos["z"]) * SIDE + pos["x"]) * 2 + core


def exchange_kernel(x_hbm, w_hbm, req_hbm, atts_hbm, attd_hbm, bias_hbm,
                    far_ref, own_hbm, q_hbm, acc_hbm, par_hbm, *scratch):
    gathered = tuple(scratch[SIDE * c:SIDE * c + SIDE] for c in range(WAYS))
    picked = scratch[SIDE * WAYS:SIDE * WAYS + WAYS]
    (x_ref, w_ref, req_ref, atts_ref, attd_ref, bias_ref, req_s, rq, rqs, own_ref, q_out, acc_out, par_ref,
     fetch_sem, give_sem,
     ask_s, ask_r, one_s, one_r, two_s, two_r, fwd_s, fwd_r, out_s, out_r, local_sem, smem_sem) = (
        scratch[SIDE * WAYS + WAYS:])
    me = lax.axis_index("node")
    core = lax.rem(me, 2)
    pos = {
        "x": lax.rem(lax.div(me, 2), SIDE),
        "z": lax.rem(lax.div(me, 2 * SIDE), SIDE),
        "y": lax.div(me, 2 * SIDE * SIDE),
    }

    def shifted(axis, off):
        return lax.rem(pos[axis] + off, SIDE)

    def device(axis, off, flip):
        where = dict(pos)
        where[axis] = shifted(axis, off)
        return place(where, lax.rem(core + flip, 2))

    def send(src, dst, ssem, rsem, axis, off, flip):
        return pltpu.make_async_remote_copy(
            src_ref=src, dst_ref=dst, send_sem=ssem, recv_sem=rsem,
            device_id=(device(axis, off, flip),), device_id_type=pl.DeviceIdType.MESH,
        )

    fetches = [
        pltpu.make_async_copy(src, dst, fetch_sem.at[i])
        for i, (src, dst) in enumerate((
            (x_hbm, x_ref), (w_hbm, w_ref), (req_hbm, req_ref), (req_hbm, req_s),
            (atts_hbm, atts_ref), (attd_hbm, attd_ref), (bias_hbm, bias_ref)))
    ]
    for f in fetches:
        f.start()
    barrier = pltpu.get_barrier_semaphore()
    for axis, off, flip in PEER_LIST:
        pl.semaphore_signal(barrier, inc=1, device_id=(device(axis, off, flip),), device_id_type=pl.DeviceIdType.MESH)
    for f in fetches:
        f.wait()

    proj = jnp.dot(x_ref[...], w_ref[...], preferred_element_type=F32).astype(BF)
    own_ref[...] = proj
    blocks = proj.reshape(NB, BLK, F)
    for c, (ga, gb, gf) in enumerate(SPLIT):
        gathered[c][0][pos[ga]] = blocks[:, ROW_AT[c]:ROW_AT[c] + SPANS[c]]

    pl.semaphore_wait(barrier, len(PEER_LIST))

    def ask(i):
        axis, off, flip = PEER_LIST[i]
        return send(req_ref, rq.at[i], ask_s.at[i], ask_r.at[i], axis, off, flip)

    def first(c, i, back=False):
        ga = SPLIT[c][0]
        off = STEPS[i]
        mine = gathered[c][0].at[pos[ga]]
        dst = gathered[c][0].at[shifted(ga, SIDE - off)] if back else mine
        return send(mine, dst, one_s.at[c, i], one_r.at[c, i], ga, off, 0)

    def second(c, k, i):
        ga, gb = SPLIT[c][:2]
        at = shifted(ga, (SIDE - TURNS[k]) % SIDE)
        return send(gathered[c][0].at[at], gathered[c][i + 1].at[at], two_s.at[c, k, i], two_r.at[c, k, i],
                    gb, STEPS[i], 0)

    def onward(c, k, i):
        ga, gb = SPLIT[c][:2]
        at = shifted(ga, (SIDE - TURNS[k]) % SIDE)
        part = pl.ds(i * (NB // 2), NB // 2)
        return send(gathered[c][i + 1].at[at, part], gathered[c][3].at[at, part], fwd_s.at[c, k, i], fwd_r.at[c, k, i],
                    gb, STEPS[i], 0)

    def landing(c, b_at, f_at, from_core):
        ga, gb, gf = SPLIT[c]
        spot = {ga: pl.ds(0, SIDE), gb: b_at, gf: f_at}
        return far_ref.at[spot["y"], spot["z"], spot["x"], from_core, pl.ds(ROW_AT[c], SPANS[c])]

    def third(c, q, j, back=False):
        ga, gb, gf = SPLIT[c]
        off, flip = LINE[j]
        b_at = shifted(gb, (SIDE - TURNS[q]) % SIDE)
        if back:
            dst = landing(c, b_at, shifted(gf, (SIDE - off) % SIDE), lax.rem(core + flip, 2))
        else:
            dst = landing(c, b_at, pos[gf], core)
        return send(picked[c].at[q, j], dst, out_s.at[c, q, j], out_r.at[c, q, j], gf, off, flip)

    def stay(c, q):
        gb, gf = SPLIT[c][1:3]
        b_at = shifted(gb, (SIDE - TURNS[q]) % SIDE)
        return pltpu.make_async_copy(picked[c].at[q, len(LINE)], landing(c, b_at, pos[gf], core), local_sem.at[c, q])

    for i in range(3):
        for c in range(WAYS):
            first(c, i).start()
    for i in range(len(PEER_LIST)):
        ask(i).start()
    for i in range(2):
        for c in range(WAYS):
            second(c, 0, i).start()

    own_head = iota((HEADS, F), 1) // HD == iota((HEADS, F), 0)

    def spread(att):
        return jnp.where(own_head, jnp.concatenate([att] * HEADS, axis=1), 0.0)

    a_s = spread(atts_ref[...])
    a_d = spread(attd_ref[...])
    own = own_ref[...]
    own_s = score_rows(stacked3(a_s), own)
    sig_col = jnp.max(own_s, axis=1, keepdims=True)
    sig_x = jnp.sum(jnp.where(own_head, sig_col, 0.0), axis=0, keepdims=True)
    par_ref[0:8] = a_s
    par_ref[8:16] = a_d
    par_ref[16:24] = jnp.broadcast_to(sig_col, (HEADS, F))
    par_ref[24:32] = jnp.broadcast_to(bias_ref[...], (8, F))
    par_ref[32:40] = jnp.broadcast_to(jnp.min(own_s - sig_col, axis=1, keepdims=True), (HEADS, F))

    same_head = iota((F, F), 0) // HD == iota((F, F), 1) // HD
    sx = nt_exact(own, jnp.where(same_head, jnp.sum(a_s, axis=0, keepdims=True), 0.0))
    dx = nt_exact(own, jnp.where(same_head, jnp.sum(a_d, axis=0, keepdims=True), 0.0))
    qx = jnp.exp(0.8 * jnp.minimum(dx + sig_x, LOW)).astype(BF)
    for h in range(HEADS):
        pick_col = (iota((F, F), 0) == h * HD).astype(F32).astype(BF)
        q_out[:, h] = jnp.dot(qx, pick_col, preferred_element_type=F32).astype(BF).reshape(NB, BLK, F)
    xo = sx - sig_x
    self_sums(acc_out, own, jnp.maximum(qx.astype(F32) * jnp.exp(xo), jnp.exp(0.2 * xo)))
    gives = [
        pltpu.make_async_copy(src, dst, give_sem.at[i])
        for i, (src, dst) in enumerate(((own_ref, own_hbm), (q_out, q_hbm), (acc_out, acc_hbm), (par_ref, par_hbm)))
    ]
    for g in gives:
        g.start()

    for k in range(1, SIDE):
        for c in range(WAYS):
            first(c, k - 1, True).wait_recv()
            for i in range(2):
                second(c, k, i).start()
    for i in range(len(PEER_LIST)):
        ask(i).wait_recv()
    fetch = pltpu.make_async_copy(rq, rqs, smem_sem.at[0])
    fetch.start()
    fetch.wait()

    def pick(c, q):
        ga, gb, gf = SPLIT[c]
        b_at = shifted(gb, (SIDE - TURNS[q]) % SIDE)
        for j in range(len(LINE) + 1):
            for a_at in range(SIDE):
                col = place({ga: a_at, gb: b_at, gf: pos[gf]}, core)
                if j < len(LINE):
                    off, flip = LINE[j]
                    block = rqs[peer_slot(gf, (SIDE - off) % SIDE, flip), 0, col]
                else:
                    block = req_s[0, col]
                picked[c][q, j, a_at] = gathered[c][q][a_at, block]

    for q in range(SIDE):
        for c in range(WAYS):
            for k in range(SIDE):
                if q in (1, 2):
                    second(c, k, q - 1).wait_recv()
                    onward(c, k, q - 1).start()
                if q == 3:
                    onward(c, k, 0).wait_recv()
                    onward(c, k, 1).wait_recv()
            pick(c, q)
            for j in range(len(LINE)):
                third(c, q, j).start()
            stay(c, q).start()

    for g in gives:
        g.wait()
    for i in range(len(PEER_LIST)):
        ask(i).wait_send()
    for c in range(WAYS):
        for i in range(3):
            first(c, i).wait_send()
        for q in range(SIDE):
            for i in range(2):
                second(c, q, i).wait_send()
                onward(c, q, i).wait_send()
    for q in range(SIDE):
        for c in range(WAYS):
            for j in range(len(LINE)):
                third(c, q, j).wait_send()
            stay(c, q).wait()
    for q in range(SIDE):
        for c in range(WAYS):
            for j in range(len(LINE)):
                third(c, q, j, True).wait_recv()


def exchange(x, weight, requests, att_src, att_dst, out_bias):
    hbm = pl.BlockSpec(memory_space=pltpu.HBM)
    dma = pltpu.SemaphoreType.DMA
    peers = len(PEER_LIST)
    lines = len(LINE)
    return pl.pallas_call(
        exchange_kernel,
        out_shape=(
            jax.ShapeDtypeStruct((SIDE, SIDE, SIDE, 2, BLK, F), BF),
            jax.ShapeDtypeStruct((NB * BLK, F), BF),
            jax.ShapeDtypeStruct((NB, HEADS, BLK, F), BF),
            jax.ShapeDtypeStruct((NB, BLK, 2 * F), F32),
            jax.ShapeDtypeStruct((40, F), F32),
        ),
        in_specs=[hbm] * 6,
        out_specs=(hbm,) * 5,
        scratch_shapes=(
            [pltpu.VMEM((SIDE, NB, span, F), BF) for span in SPANS for _ in range(SIDE)]
            + [pltpu.VMEM((SIDE, lines + 1, SIDE, span, F), BF) for span in SPANS]
            + [
                pltpu.VMEM((NB * BLK, F), BF),
                pltpu.VMEM((F, F), BF),
                pltpu.VMEM((1, PEERS), jnp.int32),
                pltpu.VMEM((HEADS, HD), F32),
                pltpu.VMEM((HEADS, HD), F32),
                pltpu.VMEM((1, F), F32),
                pltpu.SMEM((1, PEERS), jnp.int32),
                pltpu.VMEM((peers, 1, PEERS), jnp.int32),
                pltpu.SMEM((peers, 1, PEERS), jnp.int32),
                pltpu.VMEM((NB * BLK, F), BF),
                pltpu.VMEM((NB, HEADS, BLK, F), BF),
                pltpu.VMEM((NB, BLK, 2 * F), F32),
                pltpu.VMEM((40, F), F32),
                dma((7,)), dma((4,)),
                dma((peers,)), dma((peers,)),
                dma((WAYS, 3)), dma((WAYS, 3)),
                dma((WAYS, SIDE, 2)), dma((WAYS, SIDE, 2)),
                dma((WAYS, SIDE, 2)), dma((WAYS, SIDE, 2)),
                dma((WAYS, SIDE, lines)), dma((WAYS, SIDE, lines)),
                dma((WAYS, SIDE)), dma((1,)),
            ]
        ),
        compiler_params=pltpu.CompilerParams(
            collective_id=0, has_side_effects=True, vmem_limit_bytes=VMEM_ALL
        ),
        name="exchange",
    )(x, weight, requests, att_src, att_dst, out_bias.reshape(1, F))


def local(node_feats, weight, att_src, att_dst, out_bias, requests, tile_dst, tile_src, tile_masks, tile_count):
    far, own, q, sums, params = exchange(node_feats, weight, requests, att_src, att_dst, out_bias)
    far = far.reshape(PEERS, BLK, F)
    return attend(far, own, q, sums, params, tile_dst, tile_src, tile_masks[0], tile_count)


def solution(mesh):
    placed = (
        P("node", None), P(), P(), P(), P(), P("node", None), P("node", None), P("node", None),
        P("node", None, None, None), P("node"),
    )
    return jax.shard_map(local, mesh=mesh, in_specs=placed, out_specs=P("node", None), check_vma=False)
```

```python
import functools

import jax
import jax.numpy as jnp
from jax import lax
from jax.experimental import pallas as pl
from jax.experimental.pallas import tpu as pltpu
from jax.sharding import PartitionSpec as P

HEADS = 8
HD = 16
F = 128
BLK = 128
NB = 8
TILES = 128
PEERS = 128
GROUP = 16
PART = 32
J = BLK // 2
GROUPS = TILES // GROUP
VMEM_ALL = 67043328
ROWS = 16
BF = jnp.bfloat16
F32 = jnp.float32
LOW = 40.0
HIGH = 30.0
NT = (((1,), (1,)), ((), ()))


def leaky(v):
    return jnp.maximum(v, 0.2 * v)


def nt_dot(a, b):
    return lax.dot_general(a, b, NT, preferred_element_type=F32)


def split3(a):
    hi = a.astype(BF)
    r1 = a - hi.astype(F32)
    mid = r1.astype(BF)
    lo = (r1 - mid.astype(F32)).astype(BF)
    return hi, mid, lo


def nt_exact(a, b):
    hi, mid, lo = split3(b)
    return (nt_dot(a, lo) + nt_dot(a, mid)) + nt_dot(a, hi)


def stacked3(a):
    return jnp.concatenate([part.astype(F32) for part in split3(a)], axis=0).astype(BF)


def score_rows(a24, blocks):
    r = nt_dot(a24, blocks)
    return (r[16:24] + r[8:16]) + r[0:8]


def self_sums(acc, own, w):
    first_half = lax.broadcasted_iota(jnp.int32, (NB * BLK, F), 1) < F // 2
    turned = pltpu.roll(w, F // 2, 1)
    wv = w * own.astype(F32)
    acc[:, :, 0:F] = jnp.where(first_half, wv, turned).reshape(NB, BLK, F)
    acc[:, :, F:2 * F] = jnp.where(first_half, turned, wv).reshape(NB, BLK, F)


def iota(shape, dim):
    return lax.broadcasted_iota(jnp.int32, shape, dim)


def halves_joined(x):
    left = iota((HEADS, BLK), 1) < J
    turned = pltpu.roll(x, J, 1)
    zero = jnp.where(left, x, pltpu.roll(turned, HEADS - 1, 0))
    one = jnp.where(left, turned, pltpu.roll(x, HEADS - 1, 0))
    return zero, one


def half_scores(far, a24, sig_col, b_ref, d_ref, first, count, carry):
    low, high = carry
    for i in range(count // 2):
        p = first + 2 * i
        x = score_rows(a24, far[pl.ds(p, 2)].reshape(BLK, F)) - sig_col
        low = jnp.minimum(low, x)
        high = jnp.maximum(high, x)
        for ref, e in ((b_ref, jnp.exp(x)), (d_ref, jnp.exp(0.2 * x))):
            ref[p], ref[p + 1] = halves_joined(e)
    return low, high


def half_tile(k, dst, q_ref, v, m, bd_ref, head_id, ones_ref):
    cut = (BLK // ROWS, ROWS, F)
    small = (J // ROWS, ROWS, F)
    v = v.reshape(small)
    m = m.reshape(cut)
    sums = []
    for side in range(2):
        weights = []
        for pair in range(2):
            at = side * 2 + pair
            q = q_ref[dst, at].reshape(cut)
            bj = jnp.broadcast_to(bd_ref[k, 0, at][None], cut)
            dj = jnp.broadcast_to(bd_ref[k, 1, at][None], cut)
            weights.append((jnp.maximum(q * bj, dj) * m).reshape(BLK, BLK))
        values = []
        for i in range(HEADS // 2):
            h = side * (HEADS // 2) + i
            mine = jnp.broadcast_to((head_id == h)[None], small)
            values.append(jnp.where(mine, v, jnp.broadcast_to(ones_ref[h][None], small)).reshape(J, F))
        sums.append(jnp.dot(jnp.concatenate(weights, axis=1), jnp.concatenate(values, axis=0),
                            preferred_element_type=F32))
    return sums


def lane_marks(head_ref, ones_ref):
    lane_head = iota((ROWS, F), 1) // HD
    head_ref[...] = lane_head.astype(F32).astype(BF)
    for h in range(HEADS):
        ones_ref[h] = (lane_head == (h + HEADS // 2) % HEADS).astype(F32).astype(BF)


def factor_rows(k, src, b_ref, d_ref, bd_ref):
    for at in range(HEADS // 2):
        bd_ref[k, 0, at] = jnp.broadcast_to(b_ref[src, 2 * at:2 * at + 1, :], (ROWS, BLK)).astype(BF)
        bd_ref[k, 1, at] = jnp.broadcast_to(d_ref[src, 2 * at:2 * at + 1, :], (ROWS, BLK)).astype(BF)


def attend_kernel(dst_hbm, src_hbm, cnt_hbm, fara_hbm, farb_hbm, own_hbm, q_hbm, acc_hbm, par_hbm, mb_hbm, part_hbm,
                  mask_hbm, out_ref, *scratch):
    pl.run_scoped(
        functools.partial(attend_body, dst_hbm, src_hbm, cnt_hbm, fara_hbm, farb_hbm, own_hbm, q_hbm, acc_hbm, par_hbm,
                          mb_hbm, part_hbm, mask_hbm, out_ref, *scratch),
        pltpu.VMEM((NB, HEADS // 2, BLK, F), BF),
        pltpu.VMEM((PEERS, J, F), BF),
        pltpu.VMEM((GROUP, 2, HEADS // 2, ROWS, F), BF),
        pltpu.VMEM((TILES, BLK, BLK), BF),
        pltpu.VMEM((TILES, BLK, 2 * F), BF),
        pltpu.VMEM((ROWS, F), BF),
        pltpu.VMEM((HEADS, ROWS, F), BF),
    )


def attend_body(dst_hbm, src_hbm, cnt_hbm, fara_hbm, farb_hbm, own_hbm, q_hbm, acc_hbm, par_hbm, mb_hbm, part_hbm,
                mask_hbm, out_ref, masks, fara_ref, s_ref, b_ref, d_ref, acc, dmat, pmat, slog, own_ref, par_ref,
                dst_ref, src_ref, cnt_ref, far_sem, in_sem, mb_sem, part_sem, late_sem,
                q_ref, far_ref, bd_ref, m_ref, part_ref, head_ref, ones_ref):
    def far_copy(c):
        rows = pl.ds(c * PART, PART)
        return pltpu.make_async_copy(farb_hbm.at[rows], far_ref.at[rows], far_sem.at[c])

    def group_copies(g):
        rows = pl.ds(g * GROUP, GROUP)
        return (pltpu.make_async_copy(mb_hbm.at[rows], m_ref.at[rows], mb_sem.at[g]),
                pltpu.make_async_copy(part_hbm.at[rows], part_ref.at[rows], part_sem.at[g]))

    inputs = [
        pltpu.make_async_copy(src, dst, in_sem.at[i])
        for i, (src, dst) in enumerate((
            (par_hbm, par_ref), (cnt_hbm, cnt_ref), (dst_hbm, dst_ref), (src_hbm, src_ref),
            (q_hbm, q_ref), (acc_hbm, acc), (own_hbm, own_ref)))
    ]
    inputs[0].start()
    for c in range(PEERS // PART):
        far_copy(c).start()
    for copy in inputs[1:]:
        copy.start()
    for g in range(GROUPS):
        for copy in group_copies(g):
            copy.start()
    inputs[0].wait()

    a_s = par_ref[0:8]
    a_d = par_ref[8:16]
    sig_col = par_ref[16:24]
    a24 = stacked3(a_s)
    lane_marks(head_ref, ones_ref)

    def far_part(c, carry):
        far_copy(c).wait()
        return half_scores(far_ref, a24, sig_col, b_ref, d_ref, c * PART, PART, carry)

    low, high = lax.fori_loop(0, PEERS // PART, far_part, (par_ref[32:40], par_ref[40:48]))
    bounded = jnp.logical_and(jnp.min(low) >= -LOW, jnp.max(high) <= HIGH)
    for copy in inputs[1:]:
        copy.wait()
    count = cnt_ref[0, 0]
    lane1 = iota((BLK, F), 1)

    def group_wait(g, _):
        for copy in group_copies(g):
            copy.wait()
        return 0

    @pl.when(bounded)
    def _():
        live = jnp.clip((count + GROUP - 1) // GROUP, 0, GROUPS)

        def group(g, _):
            group_wait(g, 0)
            head_id = head_ref[...]
            for k in range(GROUP):
                factor_rows(k, src_ref[0, g * GROUP + k], b_ref, d_ref, bd_ref)
            for k in range(GROUP):
                t = g * GROUP + k
                dst = dst_ref[0, t]
                src = src_ref[0, t]
                sums = half_tile(k, dst, q_ref, far_ref[src], m_ref[t], bd_ref, head_id, ones_ref)
                for side in range(2):
                    cols = slice(side * F, (side + 1) * F)
                    acc[dst, :, cols] += sums[side] + part_ref[t, :, cols].astype(F32)
            return 0

        lax.fori_loop(0, live, group, 0)
        lax.fori_loop(live, GROUPS, group_wait, 0)

    @pl.when(jnp.logical_not(bounded))
    def _():
        lax.fori_loop(0, GROUPS, group_wait, 0)
        late = (pltpu.make_async_copy(mask_hbm, masks, late_sem.at[0]),
                pltpu.make_async_copy(fara_hbm, fara_ref, late_sem.at[1]))
        for copy in late:
            copy.start()
        for copy in late:
            copy.wait()
        sides = (fara_ref, far_ref)

        def raw_scores(i, _):
            for half in range(2):
                x = score_rows(a24, sides[half][pl.ds(2 * i, 2)].reshape(BLK, F))
                s_ref[half, 2 * i] = x
                s_ref[half, 2 * i + 1] = pltpu.roll(x, J, 1)
            return 0

        lax.fori_loop(0, PEERS // 2, raw_scores, 0)

        for h in range(HEADS):
            dh = jnp.broadcast_to(a_d[h:h + 1], (F, F))
            sh = jnp.broadcast_to(a_s[h:h + 1], (F, F))

            def rows(b, _):
                ob = own_ref[pl.ds(b * BLK, BLK)]
                d = nt_exact(ob, dh)
                dmat[b, h] = d
                pmat[b, h] = leaky(d + nt_exact(ob, sh))
                return 0

            lax.fori_loop(0, NB, rows, 0)

        def expand(b):
            px = pmat[b, 0]
            for h in range(1, HEADS):
                px = jnp.where(lane1 // HD == h, pmat[b, h], px)
            return px

        def keep(b, _):
            slog[pl.ds(b * BLK, BLK)] = expand(b)
            return 0

        lax.fori_loop(0, NB, keep, 0)

        def edges(t, half):
            m = masks[t].astype(F32)
            if half:
                m = pltpu.roll(m, J, 1)
            return jnp.logical_and(m > 0.5, lane1 < J)

        def peak(t, _):
            dst = dst_ref[0, t]
            src = src_ref[0, t]
            for half in range(2):
                edge = edges(t, half)
                for h in range(HEADS):
                    lg = leaky(dmat[dst, h] + s_ref[half, src, h:h + 1, :])
                    top = jnp.max(jnp.where(edge, lg, -jnp.inf), axis=1, keepdims=True)
                    pmat[dst, h] = jnp.maximum(pmat[dst, h], top)
            return 0

        lax.fori_loop(0, count, peak, 0)

        def settle(b, _):
            rows = pl.ds(b * BLK, BLK)
            slog[rows] = jnp.exp(slog[rows] - expand(b))
            return 0

        lax.fori_loop(0, NB, settle, 0)
        self_sums(acc, own_ref[...], slog[...])
        lane2 = iota((J, F), 1)

        def tile(t, _):
            dst = dst_ref[0, t]
            src = src_ref[0, t]
            for half in range(2):
                edge = edges(t, half)
                v = sides[half][src].astype(F32)
                full = jnp.concatenate([v, jnp.zeros((J, F), F32)], axis=0)
                for h in range(HEADS):
                    lg = leaky(dmat[dst, h] + s_ref[half, src, h:h + 1, :])
                    w = jnp.exp(jnp.where(edge, lg - pmat[dst, h], -jnp.inf)).astype(BF)
                    ones = jnp.where(lane1 // HD == (h + HEADS // 2) % HEADS, 1.0, 0.0)
                    r = jnp.where(lane1 // HD == h, full, ones).astype(BF)
                    at = (h // (HEADS // 2)) * F
                    acc[dst, :, at:at + F] += jnp.dot(w, r, preferred_element_type=F32)
            return 0

        lax.fori_loop(0, count, tile, 0)

    bias = par_ref[24:25]
    for b in range(NB):
        one = acc[b, :, 0:F]
        two = acc[b, :, F:2 * F]
        left = lane1 < F // 2
        top = jnp.where(left, one, two)
        low_part = pltpu.roll(jnp.where(left, two, one), F // 2, 1)
        mixed = top / low_part + bias
        small = mixed * (1.0 + mixed * (0.5 + mixed * (1.0 / 6.0 + mixed * (1.0 / 24.0))))
        neg = jnp.where(mixed > -0.0625, small, jnp.exp(jnp.minimum(mixed, 0.0)) - 1.0)
        out_ref[pl.ds(b * BLK, BLK)] = jnp.where(mixed > 0, mixed, neg).astype(BF)


def attend(dst, src, count, fara, farb, own, q, sums, params, masks_b, parts, masks):
    vm = pl.BlockSpec(memory_space=pltpu.VMEM)
    hbm = pl.BlockSpec(memory_space=pltpu.HBM)
    dma = pltpu.SemaphoreType.DMA
    return pl.pallas_call(
        attend_kernel,
        out_shape=jax.ShapeDtypeStruct((NB * BLK, F), BF),
        in_specs=[hbm] * 12,
        out_specs=vm,
        scratch_shapes=[
            pltpu.VMEM((TILES, BLK, BLK), jnp.int32),
            pltpu.VMEM((PEERS, J, F), BF),
            pltpu.VMEM((2, PEERS, HEADS, BLK), F32),
            pltpu.VMEM((PEERS, HEADS, BLK), F32),
            pltpu.VMEM((PEERS, HEADS, BLK), F32),
            pltpu.VMEM((NB, BLK, 2 * F), F32),
            pltpu.VMEM((NB, HEADS, BLK, F), F32),
            pltpu.VMEM((NB, HEADS, BLK, F), F32),
            pltpu.VMEM((NB * BLK, F), F32),
            pltpu.VMEM((NB * BLK, F), BF),
            pltpu.VMEM((48, F), F32),
            pltpu.SMEM((1, TILES), jnp.int32),
            pltpu.SMEM((1, TILES), jnp.int32),
            pltpu.SMEM((1, 1), jnp.int32),
            dma((PEERS // PART,)), dma((7,)), dma((GROUPS,)), dma((GROUPS,)), dma((2,)),
        ],
        compiler_params=pltpu.CompilerParams(vmem_limit_bytes=VMEM_ALL),
        name="attend",
    )(dst, src, count, fara, farb, own, q, sums, params, masks_b, parts, masks)


SIDE = 4
SPLIT = (("z", "y", "x"), ("x", "z", "y"), ("y", "x", "z")) * 2
ROW_AT = (0, 24, 48, 0, 24, 48)
SPANS = (24, 24, 16) * 2
WAYS = len(SPLIT)
EARLY = (0, 1, 2)
LATER = (3, 4, 5)
AXES = ("y", "z", "x")
OTHERS = tuple((off, flip) for off in (1, 3, 2) for flip in (0, 1))
LINE = ((0, 1),) + OTHERS
STEPS = (1, 3, 2)
TURNS = (0, 1, 3, 2)


def peer_list():
    peers = [("x", 0, 1)]
    for axis in AXES:
        for off, flip in OTHERS:
            peers.append((axis, off, flip))
    return peers


PEER_LIST = peer_list()


def peer_slot(axis, off, flip):
    if off == 0:
        return 0
    return PEER_LIST.index((axis, off, flip))


def place(pos, core):
    return ((pos["y"] * SIDE + pos["z"]) * SIDE + pos["x"]) * 2 + core


def exchange_kernel(x_hbm, w_hbm, req_hbm, atts_hbm, attd_hbm, bias_hbm, dst_hbm, src_hbm, cnt_hbm, mask_hbm, *refs):
    pl.run_scoped(
        functools.partial(exchange_body, x_hbm, w_hbm, req_hbm, atts_hbm, attd_hbm, bias_hbm, dst_hbm, src_hbm, cnt_hbm,
                          mask_hbm, *refs),
        pltpu.VMEM((NB, HEADS // 2, BLK, F), BF),
        pltpu.VMEM((GROUP, J, F), BF),
        pltpu.VMEM((GROUP, 2, HEADS // 2, ROWS, F), BF),
        pltpu.VMEM((TILES, BLK, BLK), BF),
        pltpu.VMEM((TILES, BLK, BLK), BF),
        pltpu.VMEM((TILES, BLK, 2 * F), BF),
        pltpu.VMEM((ROWS, F), BF),
        pltpu.VMEM((HEADS, ROWS, F), BF),
    )


def exchange_body(x_hbm, w_hbm, req_hbm, atts_hbm, attd_hbm, bias_hbm, dst_hbm, src_hbm, cnt_hbm, mask_hbm,
                  fara_hbm, farb_ref, own_hbm, q_hbm, acc_hbm, par_hbm, mb_hbm, part_hbm, *scratch):
    q_out, v_ref, bd_ref, ma_ref, mb_ref, part_ref, head_ref, ones_ref = scratch[-8:]
    scratch = scratch[:-8]
    gathered = tuple(scratch[SIDE * c:SIDE * c + SIDE] for c in range(WAYS))
    picked = scratch[SIDE * WAYS:SIDE * WAYS + WAYS]
    (x_ref, w_ref, req_ref, atts_ref, attd_ref, bias_ref, req_s, rq, rqs, own_ref, acc_out, par_ref,
     fara_ref, masks, b_ref, d_ref, dst_ref, src_ref, cnt_ref,
     fetch_sem, give_sem, mask_sem, mb_sem, part_sem,
     ask_s, ask_r, one_s, one_r, two_s, two_r, fwd_s, fwd_r, out_s, out_r, local_sem, smem_sem) = (
        scratch[SIDE * WAYS + WAYS:])
    me = lax.axis_index("node")
    core = lax.rem(me, 2)
    pos = {
        "x": lax.rem(lax.div(me, 2), SIDE),
        "z": lax.rem(lax.div(me, 2 * SIDE), SIDE),
        "y": lax.div(me, 2 * SIDE * SIDE),
    }

    def shifted(axis, off):
        return lax.rem(pos[axis] + off, SIDE)

    known = {}

    def device(axis, off, flip):
        key = (axis if off else "", off, flip)
        if key not in known:
            where = dict(pos)
            where[axis] = shifted(axis, off)
            known[key] = place(where, lax.rem(core + flip, 2))
        return known[key]

    def send(src, dst, ssem, rsem, axis, off, flip):
        return pltpu.make_async_remote_copy(
            src_ref=src, dst_ref=dst, send_sem=ssem, recv_sem=rsem,
            device_id=(device(axis, off, flip),), device_id_type=pl.DeviceIdType.MESH,
        )

    fetches = [
        pltpu.make_async_copy(src, dst, fetch_sem.at[i])
        for i, (src, dst) in enumerate((
            (x_hbm, x_ref), (w_hbm, w_ref), (req_hbm, req_ref), (req_hbm, req_s),
            (atts_hbm, atts_ref), (attd_hbm, attd_ref), (bias_hbm, bias_ref),
            (dst_hbm, dst_ref), (src_hbm, src_ref), (cnt_hbm, cnt_ref)))
    ]
    for f in fetches:
        f.start()
    barrier = pltpu.get_barrier_semaphore()
    for axis, off, flip in PEER_LIST:
        pl.semaphore_signal(barrier, inc=1, device_id=(device(axis, off, flip),), device_id_type=pl.DeviceIdType.MESH)
    for f in fetches:
        f.wait()

    proj = jnp.dot(x_ref[...], w_ref[...], preferred_element_type=F32).astype(BF)
    own_ref[...] = proj
    for c, (ga, gb, gf) in enumerate(SPLIT):
        for b in range(NB):
            at = b * BLK + (c // 3) * J + ROW_AT[c]
            gathered[c][0][pos[ga], b] = own_ref[pl.ds(at, SPANS[c])]

    pl.semaphore_wait(barrier, len(PEER_LIST))

    def ask(i):
        axis, off, flip = PEER_LIST[i]
        return send(req_ref, rq.at[i], ask_s.at[0], ask_r.at[0], axis, off, flip)

    def first(c, i, back=False):
        ga = SPLIT[c][0]
        off = STEPS[i]
        mine = gathered[c][0].at[pos[ga]]
        dst = gathered[c][0].at[shifted(ga, SIDE - off)] if back else mine
        return send(mine, dst, one_s.at[c], one_r.at[c, i], ga, off, 0)

    def second(c, k, i):
        ga, gb = SPLIT[c][:2]
        at = shifted(ga, (SIDE - TURNS[k]) % SIDE)
        return send(gathered[c][0].at[at], gathered[c][i + 1].at[at], two_s.at[c, i], two_r.at[c, k, i],
                    gb, STEPS[i], 0)

    def onward(c, k, i):
        ga, gb = SPLIT[c][:2]
        at = shifted(ga, (SIDE - TURNS[k]) % SIDE)
        part = pl.ds(i * (NB // 2), NB // 2)
        return send(gathered[c][i + 1].at[at, part], gathered[c][3].at[at, part], fwd_s.at[c, i], fwd_r.at[c],
                    gb, STEPS[i], 0)

    def landing(c, b_at, f_at, from_core):
        ga, gb, gf = SPLIT[c]
        spot = {ga: pl.ds(0, SIDE), gb: b_at, gf: f_at}
        far = farb_ref if c in LATER else fara_ref
        return far.at[spot["y"], spot["z"], spot["x"], from_core, pl.ds(ROW_AT[c], SPANS[c])]

    def third(c, q, j):
        ga, gb, gf = SPLIT[c]
        off, flip = LINE[j]
        b_at = shifted(gb, (SIDE - TURNS[q]) % SIDE)
        return send(picked[c].at[q, j], landing(c, b_at, pos[gf], core), out_s.at[c, q], out_r.at[c, q], gf, off, flip)

    def stay(c, q):
        gb, gf = SPLIT[c][1:3]
        b_at = shifted(gb, (SIDE - TURNS[q]) % SIDE)
        return pltpu.make_async_copy(picked[c].at[q, len(LINE)], landing(c, b_at, pos[gf], core), local_sem.at[c, q])

    def bulk(ref, ssem, rsem):
        return send(ref, ref, ssem, rsem, "x", 0, 1)

    def all_asks():
        return bulk(rq, ask_s.at[0], ask_r.at[0])

    def all_onward(c):
        return bulk(gathered[c][3], fwd_s.at[c, 0], fwd_r.at[c])

    def all_third(c, q):
        return bulk(picked[c].at[q, pl.ds(0, len(LINE))], out_s.at[c, q], out_r.at[c, q])

    def mask_copy(g):
        rows = pl.ds(g * GROUP, GROUP)
        return pltpu.make_async_copy(mask_hbm.at[rows], masks.at[rows], mask_sem.at[g])

    def group_gives(g):
        rows = pl.ds(g * GROUP, GROUP)
        return (pltpu.make_async_copy(mb_ref.at[rows], mb_hbm.at[rows], mb_sem.at[g]),
                pltpu.make_async_copy(part_ref.at[rows], part_hbm.at[rows], part_sem.at[g]))

    for i in range(3):
        for c in EARLY:
            first(c, i).start()
    for i in range(len(PEER_LIST)):
        ask(i).start()
    for i in range(2):
        for c in EARLY:
            second(c, 0, i).start()
    for i in range(3):
        for c in LATER:
            first(c, i).start()
    for g in range(GROUPS):
        mask_copy(g).start()

    own_head = iota((HEADS, F), 1) // HD == iota((HEADS, F), 0)

    def spread(att):
        return jnp.where(own_head, jnp.concatenate([att] * HEADS, axis=1), 0.0)

    a_s = spread(atts_ref[...])
    a_d = spread(attd_ref[...])
    own = own_ref[...]
    a24 = stacked3(a_s)
    own_s = score_rows(a24, own)
    sig_col = jnp.max(own_s, axis=1, keepdims=True)
    sig_x = jnp.sum(jnp.where(own_head, sig_col, 0.0), axis=0, keepdims=True)
    par_ref[0:8] = a_s
    par_ref[8:16] = a_d
    par_ref[16:24] = jnp.broadcast_to(sig_col, (HEADS, F))
    par_ref[24:32] = jnp.broadcast_to(bias_ref[...], (8, F))
    own_low = jnp.broadcast_to(jnp.min(own_s - sig_col, axis=1, keepdims=True), (HEADS, F))

    same_head = iota((F, F), 0) // HD == iota((F, F), 1) // HD
    sx = nt_exact(own, jnp.where(same_head, jnp.sum(a_s, axis=0, keepdims=True), 0.0))
    dx = nt_exact(own, jnp.where(same_head, jnp.sum(a_d, axis=0, keepdims=True), 0.0))
    qx = jnp.exp(0.8 * jnp.minimum(dx + sig_x, LOW)).astype(BF)
    for h in range(HEADS // 2):
        wanted_row = (2 * h + iota((F, F), 1) // J) * HD
        pick_col = (iota((F, F), 0) == wanted_row).astype(F32).astype(BF)
        q_out[:, h] = jnp.dot(qx, pick_col, preferred_element_type=F32).astype(BF).reshape(NB, BLK, F)
    xo = sx - sig_x
    self_sums(acc_out, own, jnp.maximum(qx.astype(F32) * jnp.exp(xo), jnp.exp(0.2 * xo)))
    gives = [
        pltpu.make_async_copy(src, dst, give_sem.at[i])
        for i, (src, dst) in enumerate(((own_ref, own_hbm), (q_out, q_hbm), (acc_out, acc_hbm)))
    ]
    for g in gives:
        g.start()

    def spread_second(ways):
        for k in range(1, SIDE):
            for c in ways:
                first(c, k - 1, True).wait_recv()
                for i in range(2):
                    second(c, k, i).start()

    spread_second(EARLY)
    for i in range(2):
        for c in LATER:
            second(c, 0, i).start()
    all_asks().wait_recv()
    fetch = pltpu.make_async_copy(rq, rqs, smem_sem.at[0])
    fetch.start()
    fetch.wait()

    def pick(c, q):
        ga, gb, gf = SPLIT[c]
        b_at = shifted(gb, (SIDE - TURNS[q]) % SIDE)
        for j in range(len(LINE) + 1):
            for a_at in range(SIDE):
                col = place({ga: a_at, gb: b_at, gf: pos[gf]}, core)
                if j < len(LINE):
                    off, flip = LINE[j]
                    block = rqs[peer_slot(gf, (SIDE - off) % SIDE, flip), 0, col]
                else:
                    block = req_s[0, col]
                part = gathered[c][q][a_at, block]
                if c in EARLY and j == len(LINE):
                    spot = {ga: a_at, gb: b_at, gf: pos[gf]}
                    fara_ref[spot["y"], spot["z"], spot["x"], core, pl.ds(ROW_AT[c], SPANS[c])] = part
                else:
                    picked[c][q, j, a_at] = part

    count = cnt_ref[0, 0]
    left = iota((BLK, BLK), 1) < J
    lane_marks(head_ref, ones_ref)

    def prepare(g, _):
        mask_copy(g).wait()
        for k in range(GROUP):
            t = g * GROUP + k
            m = masks[t].astype(F32) * (t < count).astype(F32)
            turned = pltpu.roll(m, J, 1)
            ma_ref[t] = jnp.where(left, m, turned).astype(BF)
            mb_ref[t] = jnp.where(left, turned, m).astype(BF)
        group_gives(g)[0].start()
        return 0

    def pass_on(c, q):
        for k in range(SIDE):
            second(c, k, q - 1).wait_recv()
            onward(c, k, q - 1).start()

    def hand_out(c, q):
        pick(c, q)
        for j in range(len(LINE)):
            third(c, q, j).start()
        if c in LATER:
            stay(c, q).start()

    for c in EARLY:
        hand_out(c, 0)
    lax.fori_loop(0, GROUPS // 2, prepare, 0)
    spread_second(LATER)
    for q in (1, 2):
        for c in EARLY:
            pass_on(c, q)
            hand_out(c, q)
    lax.fori_loop(GROUPS // 2, GROUPS, prepare, 0)
    for c in EARLY:
        all_onward(c).wait_recv()
        hand_out(c, 3)
    for q in (1, 2):
        for c in LATER:
            pass_on(c, q)
    for q in (0, 1, 2):
        for c in LATER:
            hand_out(c, q)
    for c in LATER:
        all_onward(c).wait_recv()
        hand_out(c, 3)

    for q in range(SIDE):
        for c in EARLY:
            all_third(c, q).wait_recv()

    def far_part(c, carry):
        p = c * PART
        return half_scores(fara_flat, a24, sig_col, b_ref, d_ref, p, PART, carry)

    fara_flat = fara_ref.reshape(PEERS, J, F)
    low, high = lax.fori_loop(0, PEERS // PART, far_part, (own_low, jnp.zeros((HEADS, F), F32)))
    par_ref[32:40] = low
    par_ref[40:48] = high
    last = (pltpu.make_async_copy(par_ref, par_hbm, give_sem.at[3]),
            pltpu.make_async_copy(fara_ref, fara_hbm, give_sem.at[4]))
    for copy in last:
        copy.start()

    def group(g, _):
        head_id = head_ref[...]
        for k in range(GROUP):
            src = src_ref[0, g * GROUP + k]
            v_ref[k] = fara_flat[src]
            factor_rows(k, src, b_ref, d_ref, bd_ref)
        for k in range(GROUP):
            t = g * GROUP + k
            sums = half_tile(k, dst_ref[0, t], q_out, v_ref[k], ma_ref[t], bd_ref, head_id, ones_ref)
            for side in range(2):
                part_ref[t, :, side * F:(side + 1) * F] = sums[side].astype(BF)
        group_gives(g)[1].start()
        return 0

    lax.fori_loop(0, GROUPS, group, 0)

    for g in gives:
        g.wait()
    for copy in last:
        copy.wait()
    all_asks().wait_send()
    for c in range(WAYS):
        bulk(gathered[c][0].at[pl.ds(0, 3)], one_s.at[c], one_r.at[c, 0]).wait_send()
        for i in range(2):
            bulk(gathered[c][i + 1], two_s.at[c, i], two_r.at[c, 0, 0]).wait_send()
            bulk(gathered[c][3].at[:, pl.ds(0, NB // 2)], fwd_s.at[c, i], fwd_r.at[c]).wait_send()
    for g in range(GROUPS):
        for copy in group_gives(g):
            copy.wait()
    for q in range(SIDE):
        for c in range(WAYS):
            all_third(c, q).wait_send()
        for c in LATER:
            stay(c, q).wait()
    for q in range(SIDE):
        for c in LATER:
            all_third(c, q).wait_recv()


def exchange(x, weight, requests, att_src, att_dst, out_bias, dst, src, count, masks):
    hbm = pl.BlockSpec(memory_space=pltpu.HBM)
    dma = pltpu.SemaphoreType.DMA
    peers = len(PEER_LIST)
    lines = len(LINE)
    far = (SIDE, SIDE, SIDE, 2, J, F)
    return pl.pallas_call(
        exchange_kernel,
        out_shape=(
            jax.ShapeDtypeStruct(far, BF),
            jax.ShapeDtypeStruct(far, BF),
            jax.ShapeDtypeStruct((NB * BLK, F), BF),
            jax.ShapeDtypeStruct((NB, HEADS // 2, BLK, F), BF),
            jax.ShapeDtypeStruct((NB, BLK, 2 * F), F32),
            jax.ShapeDtypeStruct((48, F), F32),
            jax.ShapeDtypeStruct((TILES, BLK, BLK), BF),
            jax.ShapeDtypeStruct((TILES, BLK, 2 * F), BF),
        ),
        in_specs=[hbm] * 10,
        out_specs=(hbm,) * 8,
        scratch_shapes=(
            [pltpu.VMEM((SIDE, NB, span, F), BF) for span in SPANS for _ in range(SIDE)]
            + [pltpu.VMEM((SIDE, lines + 1, SIDE, span, F), BF) for span in SPANS]
            + [
                pltpu.VMEM((NB * BLK, F), BF),
                pltpu.VMEM((F, F), BF),
                pltpu.VMEM((1, PEERS), jnp.int32),
                pltpu.VMEM((HEADS, HD), F32),
                pltpu.VMEM((HEADS, HD), F32),
                pltpu.VMEM((1, F), F32),
                pltpu.SMEM((1, PEERS), jnp.int32),
                pltpu.VMEM((peers, 1, PEERS), jnp.int32),
                pltpu.SMEM((peers, 1, PEERS), jnp.int32),
                pltpu.VMEM((NB * BLK, F), BF),
                pltpu.VMEM((NB, BLK, 2 * F), F32),
                pltpu.VMEM((48, F), F32),
                pltpu.VMEM(far, BF),
                pltpu.VMEM((TILES, BLK, BLK), jnp.int32),
                pltpu.VMEM((PEERS, HEADS, BLK), F32),
                pltpu.VMEM((PEERS, HEADS, BLK), F32),
                pltpu.SMEM((1, TILES), jnp.int32),
                pltpu.SMEM((1, TILES), jnp.int32),
                pltpu.SMEM((1, 1), jnp.int32),
                dma((10,)), dma((5,)), dma((GROUPS,)), dma((GROUPS,)), dma((GROUPS,)),
                dma((1,)), dma((1,)),
                dma((WAYS,)), dma((WAYS, 3)),
                dma((WAYS, 2)), dma((WAYS, SIDE, 2)),
                dma((WAYS, 2)), dma((WAYS,)),
                dma((WAYS, SIDE)), dma((WAYS, SIDE)),
                dma((WAYS, SIDE)), dma((1,)),
            ]
        ),
        compiler_params=pltpu.CompilerParams(
            collective_id=0, has_side_effects=True, vmem_limit_bytes=VMEM_ALL
        ),
        name="exchange",
    )(x, weight, requests, att_src, att_dst, out_bias.reshape(1, F), dst, src, count, masks)


def local(node_feats, weight, att_src, att_dst, out_bias, requests, tile_dst, tile_src, tile_masks, tile_count):
    count = tile_count.reshape(1, 1)
    masks = tile_masks[0]
    fara, farb, *rest = exchange(node_feats, weight, requests, att_src, att_dst, out_bias, tile_dst, tile_src, count, masks)
    fara = fara.reshape(PEERS, J, F)
    farb = farb.reshape(PEERS, J, F)
    return attend(tile_dst, tile_src, count, fara, farb, *rest, masks)


def solution(mesh):
    placed = (
        P("node", None), P(), P(), P(), P(), P("node", None), P("node", None), P("node", None),
        P("node", None, None, None), P("node"),
    )
    return jax.shard_map(local, mesh=mesh, in_specs=placed, out_specs=P("node", None), check_vma=False)
```

```python
import functools

import jax
import jax.numpy as jnp
from jax import lax
from jax.experimental import pallas as pl
from jax.experimental.pallas import tpu as pltpu
from jax.sharding import PartitionSpec as P

HEADS = 8
HD = 16
F = 128
BLK = 128
NB = 8
TILES = 128
PEERS = 128
GROUP = 32
PART = 32
J = BLK // 2
GROUPS = TILES // GROUP
VMEM_ALL = 67043328
ROWS = 16
BF = jnp.bfloat16
F32 = jnp.float32
LOW = 40.0
HIGH = 30.0
NT = (((1,), (1,)), ((), ()))


def leaky(v):
    return jnp.maximum(v, 0.2 * v)


def nt_dot(a, b):
    return lax.dot_general(a, b, NT, preferred_element_type=F32)


def split3(a):
    hi = a.astype(BF)
    r1 = a - hi.astype(F32)
    mid = r1.astype(BF)
    lo = (r1 - mid.astype(F32)).astype(BF)
    return hi, mid, lo


def nt_exact(a, b):
    hi, mid, lo = split3(b)
    return (nt_dot(a, lo) + nt_dot(a, mid)) + nt_dot(a, hi)


def stacked3(a):
    return jnp.concatenate([part.astype(F32) for part in split3(a)], axis=0).astype(BF)


def score_rows(a24, blocks):
    r = nt_dot(a24, blocks)
    return (r[16:24] + r[8:16]) + r[0:8]


def self_sums(acc, own, w):
    first_half = lax.broadcasted_iota(jnp.int32, (NB * BLK, F), 1) < F // 2
    turned = pltpu.roll(w, F // 2, 1)
    wv = w * own.astype(F32)
    acc[:, :, 0:F] = jnp.where(first_half, wv, turned).reshape(NB, BLK, F)
    acc[:, :, F:2 * F] = jnp.where(first_half, turned, wv).reshape(NB, BLK, F)


def iota(shape, dim):
    return lax.broadcasted_iota(jnp.int32, shape, dim)


def halves_joined(x):
    left = iota((HEADS, BLK), 1) < J
    turned = pltpu.roll(x, J, 1)
    zero = jnp.where(left, x, pltpu.roll(turned, HEADS - 1, 0))
    one = jnp.where(left, turned, pltpu.roll(x, HEADS - 1, 0))
    return zero, one


def half_scores(far, a24, sig_col, b_ref, d_ref, first, count, carry):
    low, high = carry
    for i in range(count // 2):
        p = first + 2 * i
        x = score_rows(a24, far[pl.ds(p, 2)].reshape(BLK, F)) - sig_col
        low = jnp.minimum(low, x)
        high = jnp.maximum(high, x)
        for ref, e in ((b_ref, jnp.exp(x)), (d_ref, jnp.exp(0.2 * x))):
            ref[p], ref[p + 1] = halves_joined(e)
    return low, high


def half_tile(k, dst, q_ref, v, m, bd_ref, head_id, ones_ref):
    cut = (BLK // ROWS, ROWS, F)
    small = (J // ROWS, ROWS, F)
    v = v.reshape(small)
    m = m.reshape(cut)
    w_rows, v_cols = [], []
    for side in range(2):
        weights = []
        for pair in range(2):
            at = side * 2 + pair
            q = q_ref[dst, at].reshape(cut)
            bj = jnp.broadcast_to(bd_ref[k, 0, at][None], cut)
            dj = jnp.broadcast_to(bd_ref[k, 1, at][None], cut)
            weights.append((jnp.maximum(q * bj, dj) * m).reshape(BLK, BLK))
        values = []
        for i in range(HEADS // 2):
            h = side * (HEADS // 2) + i
            mine = jnp.broadcast_to((head_id == h)[None], small)
            values.append(jnp.where(mine, v, jnp.broadcast_to(ones_ref[h][None], small)).reshape(J, F))
        w_rows.append(jnp.concatenate(weights, axis=1))
        v_cols.append(jnp.concatenate(values, axis=0))
    o = jnp.dot(jnp.concatenate(w_rows, axis=0), jnp.concatenate(v_cols, axis=1), preferred_element_type=F32)
    return o[0:BLK, 0:F], o[BLK:2 * BLK, F:2 * F]


def lane_marks(head_ref, ones_ref):
    lane_head = iota((ROWS, F), 1) // HD
    head_ref[...] = lane_head.astype(F32).astype(BF)
    for h in range(HEADS):
        ones_ref[h] = (lane_head == (h + HEADS // 2) % HEADS).astype(F32).astype(BF)


def factor_rows(k, src, b_ref, d_ref, bd_ref):
    for at in range(HEADS // 2):
        bd_ref[k, 0, at] = jnp.broadcast_to(b_ref[src, 2 * at:2 * at + 1, :], (ROWS, BLK)).astype(BF)
        bd_ref[k, 1, at] = jnp.broadcast_to(d_ref[src, 2 * at:2 * at + 1, :], (ROWS, BLK)).astype(BF)


def attend_kernel(dst_hbm, src_hbm, cnt_hbm, fara_hbm, farb_hbm, own_hbm, q_hbm, acc_hbm, par_hbm, mb_hbm, part_hbm,
                  mask_hbm, out_ref, *scratch):
    pl.run_scoped(
        functools.partial(attend_body, dst_hbm, src_hbm, cnt_hbm, fara_hbm, farb_hbm, own_hbm, q_hbm, acc_hbm, par_hbm,
                          mb_hbm, part_hbm, mask_hbm, out_ref, *scratch),
        pltpu.VMEM((NB, HEADS // 2, BLK, F), BF),
        pltpu.VMEM((PEERS, J, F), BF),
        pltpu.VMEM((GROUP, 2, HEADS // 2, ROWS, F), BF),
        pltpu.VMEM((TILES, BLK, BLK), BF),
        pltpu.VMEM((TILES, BLK, 2 * F), BF),
        pltpu.VMEM((ROWS, F), BF),
        pltpu.VMEM((HEADS, ROWS, F), BF),
    )


def attend_body(dst_hbm, src_hbm, cnt_hbm, fara_hbm, farb_hbm, own_hbm, q_hbm, acc_hbm, par_hbm, mb_hbm, part_hbm,
                mask_hbm, out_ref, masks, fara_ref, s_ref, b_ref, d_ref, acc, self_ref, dmat, pmat, slog, own_ref, par_ref,
                dst_ref, src_ref, cnt_ref, far_sem, in_sem, mb_sem, part_sem, late_sem,
                q_ref, far_ref, bd_ref, m_ref, part_ref, head_ref, ones_ref):
    def far_copy(c):
        rows = pl.ds(c * PART, PART)
        return pltpu.make_async_copy(farb_hbm.at[rows], far_ref.at[rows], far_sem.at[c])

    def group_copies(g):
        rows = pl.ds(g * GROUP, GROUP)
        return (pltpu.make_async_copy(mb_hbm.at[rows], m_ref.at[rows], mb_sem.at[g]),
                pltpu.make_async_copy(part_hbm.at[rows], part_ref.at[rows], part_sem.at[g]))

    inputs = [
        pltpu.make_async_copy(src, dst, in_sem.at[i])
        for i, (src, dst) in enumerate((
            (par_hbm, par_ref), (cnt_hbm, cnt_ref), (dst_hbm, dst_ref), (src_hbm, src_ref),
            (q_hbm, q_ref)))
    ]
    inputs[0].start()
    for c in range(PEERS // PART):
        far_copy(c).start()
    for copy in inputs[1:]:
        copy.start()
    self_copy = pltpu.make_async_copy(acc_hbm, self_ref, late_sem.at[2])
    for g in range(GROUPS):
        for copy in group_copies(g):
            copy.start()
        if g == 0:
            self_copy.start()
    acc[...] = jnp.zeros_like(acc)
    inputs[0].wait()

    a_s = par_ref[0:8]
    a_d = par_ref[8:16]
    sig_col = par_ref[16:24]
    a24 = stacked3(a_s)
    lane_marks(head_ref, ones_ref)

    def far_part(c, carry):
        far_copy(c).wait()
        return half_scores(far_ref, a24, sig_col, b_ref, d_ref, c * PART, PART, carry)

    low, high = lax.fori_loop(0, PEERS // PART, far_part, (par_ref[32:40], par_ref[40:48]))
    bounded = jnp.logical_and(jnp.min(low) >= -LOW, jnp.max(high) <= HIGH)
    for copy in inputs[1:]:
        copy.wait()
    count = cnt_ref[0, 0]
    lane1 = iota((BLK, F), 1)

    def group_wait(g, _):
        for copy in group_copies(g):
            copy.wait()
        return 0

    @pl.when(bounded)
    def _():
        live = jnp.clip((count + GROUP - 1) // GROUP, 0, GROUPS)

        def group(g, _):
            group_wait(g, 0)
            head_id = head_ref[...]
            for k in range(GROUP):
                factor_rows(k, src_ref[0, g * GROUP + k], b_ref, d_ref, bd_ref)
            for k in range(GROUP):
                t = g * GROUP + k
                dst = dst_ref[0, t]
                src = src_ref[0, t]
                sums = half_tile(k, dst, q_ref, far_ref[src], m_ref[t], bd_ref, head_id, ones_ref)
                for side in range(2):
                    cols = slice(side * F, (side + 1) * F)
                    acc[dst, :, cols] += sums[side] + part_ref[t, :, cols].astype(F32)
            return 0

        lax.fori_loop(0, live, group, 0)
        lax.fori_loop(live, GROUPS, group_wait, 0)
        self_copy.wait()

    @pl.when(jnp.logical_not(bounded))
    def _():
        lax.fori_loop(0, GROUPS, group_wait, 0)
        self_copy.wait()
        late = (pltpu.make_async_copy(mask_hbm, masks, late_sem.at[0]),
                pltpu.make_async_copy(fara_hbm, fara_ref, late_sem.at[1]),
                pltpu.make_async_copy(own_hbm, own_ref, late_sem.at[3]))
        for copy in late:
            copy.start()
        for copy in late:
            copy.wait()
        sides = (fara_ref, far_ref)

        def raw_scores(i, _):
            for half in range(2):
                x = score_rows(a24, sides[half][pl.ds(2 * i, 2)].reshape(BLK, F))
                s_ref[half, 2 * i] = x
                s_ref[half, 2 * i + 1] = pltpu.roll(x, J, 1)
            return 0

        lax.fori_loop(0, PEERS // 2, raw_scores, 0)

        for h in range(HEADS):
            dh = jnp.broadcast_to(a_d[h:h + 1], (F, F))
            sh = jnp.broadcast_to(a_s[h:h + 1], (F, F))

            def rows(b, _):
                ob = own_ref[pl.ds(b * BLK, BLK)]
                d = nt_exact(ob, dh)
                dmat[b, h] = d
                pmat[b, h] = leaky(d + nt_exact(ob, sh))
                return 0

            lax.fori_loop(0, NB, rows, 0)

        def expand(b):
            px = pmat[b, 0]
            for h in range(1, HEADS):
                px = jnp.where(lane1 // HD == h, pmat[b, h], px)
            return px

        def keep(b, _):
            slog[pl.ds(b * BLK, BLK)] = expand(b)
            return 0

        lax.fori_loop(0, NB, keep, 0)

        def edges(t, half):
            m = masks[t].astype(F32)
            if half:
                m = pltpu.roll(m, J, 1)
            return jnp.logical_and(m > 0.5, lane1 < J)

        def peak(t, _):
            dst = dst_ref[0, t]
            src = src_ref[0, t]
            for half in range(2):
                edge = edges(t, half)
                for h in range(HEADS):
                    lg = leaky(dmat[dst, h] + s_ref[half, src, h:h + 1, :])
                    top = jnp.max(jnp.where(edge, lg, -jnp.inf), axis=1, keepdims=True)
                    pmat[dst, h] = jnp.maximum(pmat[dst, h], top)
            return 0

        lax.fori_loop(0, count, peak, 0)

        def settle(b, _):
            rows = pl.ds(b * BLK, BLK)
            slog[rows] = jnp.exp(slog[rows] - expand(b))
            return 0

        lax.fori_loop(0, NB, settle, 0)
        self_sums(self_ref, own_ref[...], slog[...])
        lane2 = iota((J, F), 1)

        def tile(t, _):
            dst = dst_ref[0, t]
            src = src_ref[0, t]
            for half in range(2):
                edge = edges(t, half)
                v = sides[half][src].astype(F32)
                full = jnp.concatenate([v, jnp.zeros((J, F), F32)], axis=0)
                for h in range(HEADS):
                    lg = leaky(dmat[dst, h] + s_ref[half, src, h:h + 1, :])
                    w = jnp.exp(jnp.where(edge, lg - pmat[dst, h], -jnp.inf)).astype(BF)
                    ones = jnp.where(lane1 // HD == (h + HEADS // 2) % HEADS, 1.0, 0.0)
                    r = jnp.where(lane1 // HD == h, full, ones).astype(BF)
                    at = (h // (HEADS // 2)) * F
                    acc[dst, :, at:at + F] += jnp.dot(w, r, preferred_element_type=F32)
            return 0

        lax.fori_loop(0, count, tile, 0)

    bias = par_ref[24:25]
    for b in range(NB):
        one = acc[b, :, 0:F] + self_ref[b, :, 0:F]
        two = acc[b, :, F:2 * F] + self_ref[b, :, F:2 * F]
        left = lane1 < F // 2
        top = jnp.where(left, one, two)
        low_part = pltpu.roll(jnp.where(left, two, one), F // 2, 1)
        mixed = top / low_part + bias
        small = mixed * (1.0 + mixed * (0.5 + mixed * (1.0 / 6.0 + mixed * (1.0 / 24.0))))
        neg = jnp.where(mixed > -0.0625, small, jnp.exp(jnp.minimum(mixed, 0.0)) - 1.0)
        out_ref[pl.ds(b * BLK, BLK)] = jnp.where(mixed > 0, mixed, neg).astype(BF)


def attend(dst, src, count, fara, farb, own, q, sums, params, masks_b, parts, masks):
    vm = pl.BlockSpec(memory_space=pltpu.VMEM)
    hbm = pl.BlockSpec(memory_space=pltpu.HBM)
    dma = pltpu.SemaphoreType.DMA
    return pl.pallas_call(
        attend_kernel,
        out_shape=jax.ShapeDtypeStruct((NB * BLK, F), BF),
        in_specs=[hbm] * 12,
        out_specs=vm,
        scratch_shapes=[
            pltpu.VMEM((TILES, BLK, BLK), jnp.int32),
            pltpu.VMEM((PEERS, J, F), BF),
            pltpu.VMEM((2, PEERS, HEADS, BLK), F32),
            pltpu.VMEM((PEERS, HEADS, BLK), F32),
            pltpu.VMEM((PEERS, HEADS, BLK), F32),
            pltpu.VMEM((NB, BLK, 2 * F), F32),
            pltpu.VMEM((NB, BLK, 2 * F), F32),
            pltpu.VMEM((NB, HEADS, BLK, F), F32),
            pltpu.VMEM((NB, HEADS, BLK, F), F32),
            pltpu.VMEM((NB * BLK, F), F32),
            pltpu.VMEM((NB * BLK, F), BF),
            pltpu.VMEM((48, F), F32),
            pltpu.SMEM((1, TILES), jnp.int32),
            pltpu.SMEM((1, TILES), jnp.int32),
            pltpu.SMEM((1, 1), jnp.int32),
            dma((PEERS // PART,)), dma((5,)), dma((GROUPS,)), dma((GROUPS,)), dma((4,)),
        ],
        compiler_params=pltpu.CompilerParams(vmem_limit_bytes=VMEM_ALL),
        name="attend",
    )(dst, src, count, fara, farb, own, q, sums, params, masks_b, parts, masks)


SIDE = 4
SPLIT = (("z", "y", "x"), ("x", "z", "y"), ("y", "x", "z"), ("y", "z", "x"), ("z", "x", "y"), ("x", "y", "z"))
ROW_AT = (0, 24, 48, 0, 24, 40)
SPANS = (24, 24, 16, 24, 16, 24)
WAYS = len(SPLIT)
EARLY = (0, 1, 2)
LATER = (3, 4, 5)
AXES = ("y", "z", "x")
OTHERS = tuple((off, flip) for off in (1, 3, 2) for flip in (0, 1))
LINE = ((0, 1),) + OTHERS
STEPS = (1, 3, 2)
TURNS = (0, 1, 3, 2)


def peer_list():
    peers = [("x", 0, 1)]
    for axis in AXES:
        for off, flip in OTHERS:
            peers.append((axis, off, flip))
    return peers


PEER_LIST = peer_list()


def peer_slot(axis, off, flip):
    if off == 0:
        return 0
    return PEER_LIST.index((axis, off, flip))


def place(pos, core):
    return ((pos["y"] * SIDE + pos["z"]) * SIDE + pos["x"]) * 2 + core


def exchange_kernel(x_hbm, w_hbm, req_hbm, atts_hbm, attd_hbm, bias_hbm, dst_hbm, src_hbm, cnt_hbm, mask_hbm, *refs):
    pl.run_scoped(
        functools.partial(exchange_body, x_hbm, w_hbm, req_hbm, atts_hbm, attd_hbm, bias_hbm, dst_hbm, src_hbm, cnt_hbm,
                          mask_hbm, *refs),
        pltpu.VMEM((NB, HEADS // 2, BLK, F), BF),
        pltpu.VMEM((GROUP, J, F), BF),
        pltpu.VMEM((GROUP, 2, HEADS // 2, ROWS, F), BF),
        pltpu.VMEM((TILES, BLK, BLK), BF),
        pltpu.VMEM((TILES, BLK, BLK), BF),
        pltpu.VMEM((TILES, BLK, 2 * F), BF),
        pltpu.VMEM((ROWS, F), BF),
        pltpu.VMEM((HEADS, ROWS, F), BF),
    )


def exchange_body(x_hbm, w_hbm, req_hbm, atts_hbm, attd_hbm, bias_hbm, dst_hbm, src_hbm, cnt_hbm, mask_hbm,
                  fara_hbm, farb_ref, own_hbm, q_hbm, acc_hbm, par_hbm, mb_hbm, part_hbm, *scratch):
    q_out, v_ref, bd_ref, ma_ref, mb_ref, part_ref, head_ref, ones_ref = scratch[-8:]
    scratch = scratch[:-8]
    gathered = tuple(scratch[SIDE * c:SIDE * c + SIDE] for c in range(WAYS))
    picked = scratch[SIDE * WAYS:SIDE * WAYS + WAYS]
    (x_ref, w_ref, req_ref, atts_ref, attd_ref, bias_ref, req_s, rq, rqs, own_ref, acc_out, par_ref,
     fara_ref, masks, b_ref, d_ref, dst_ref, src_ref, cnt_ref,
     fetch_sem, give_sem, mask_sem, mb_sem, part_sem,
     ask_s, ask_r, one_s, one_r, two_s, two_r, fwd_s, fwd_r, out_s, out_r, local_sem, smem_sem) = (
        scratch[SIDE * WAYS + WAYS:])
    me = lax.axis_index("node")
    core = lax.rem(me, 2)
    pos = {
        "x": lax.rem(lax.div(me, 2), SIDE),
        "z": lax.rem(lax.div(me, 2 * SIDE), SIDE),
        "y": lax.div(me, 2 * SIDE * SIDE),
    }

    def shifted(axis, off):
        return lax.rem(pos[axis] + off, SIDE)

    known = {}

    def device(axis, off, flip):
        key = (axis if off else "", off, flip)
        if key not in known:
            where = dict(pos)
            where[axis] = shifted(axis, off)
            known[key] = place(where, lax.rem(core + flip, 2))
        return known[key]

    def send(src, dst, ssem, rsem, axis, off, flip):
        return pltpu.make_async_remote_copy(
            src_ref=src, dst_ref=dst, send_sem=ssem, recv_sem=rsem,
            device_id=(device(axis, off, flip),), device_id_type=pl.DeviceIdType.MESH,
        )

    fetches = [
        pltpu.make_async_copy(src, dst, fetch_sem.at[i])
        for i, (src, dst) in enumerate((
            (x_hbm, x_ref), (w_hbm, w_ref), (req_hbm, req_ref), (req_hbm, req_s),
            (atts_hbm, atts_ref), (attd_hbm, attd_ref), (bias_hbm, bias_ref),
            (dst_hbm, dst_ref), (src_hbm, src_ref), (cnt_hbm, cnt_ref)))
    ]
    for f in fetches:
        f.start()
    barrier = pltpu.get_barrier_semaphore()
    for axis, off, flip in PEER_LIST:
        pl.semaphore_signal(barrier, inc=1, device_id=(device(axis, off, flip),), device_id_type=pl.DeviceIdType.MESH)
    for f in fetches:
        f.wait()

    proj = jnp.dot(x_ref[...], w_ref[...], preferred_element_type=F32).astype(BF)
    own_ref[...] = proj
    for c, (ga, gb, gf) in enumerate(SPLIT):
        for b in range(NB):
            at = b * BLK + (c // 3) * J + ROW_AT[c]
            gathered[c][0][pos[ga], b] = own_ref[pl.ds(at, SPANS[c])]

    pl.semaphore_wait(barrier, len(PEER_LIST))

    def ask(i):
        axis, off, flip = PEER_LIST[i]
        return send(req_ref, rq.at[i], ask_s.at[0], ask_r.at[0], axis, off, flip)

    def first(c, i, back=False):
        ga = SPLIT[c][0]
        off = STEPS[i]
        mine = gathered[c][0].at[pos[ga]]
        dst = gathered[c][0].at[shifted(ga, SIDE - off)] if back else mine
        return send(mine, dst, one_s.at[c], one_r.at[c, i], ga, off, 0)

    def second(c, k, i):
        ga, gb = SPLIT[c][:2]
        at = shifted(ga, (SIDE - TURNS[k]) % SIDE)
        return send(gathered[c][0].at[at], gathered[c][i + 1].at[at], two_s.at[c, i], two_r.at[c, k, i],
                    gb, STEPS[i], 0)

    def onward(c, k, i):
        ga, gb = SPLIT[c][:2]
        at = shifted(ga, (SIDE - TURNS[k]) % SIDE)
        part = pl.ds(i * (NB // 2), NB // 2)
        return send(gathered[c][i + 1].at[at, part], gathered[c][3].at[at, part], fwd_s.at[c, i], fwd_r.at[c],
                    gb, STEPS[i], 0)

    def landing(c, b_at, f_at, from_core):
        ga, gb, gf = SPLIT[c]
        spot = {ga: pl.ds(0, SIDE), gb: b_at, gf: f_at}
        far = farb_ref if c in LATER else fara_ref
        return far.at[spot["y"], spot["z"], spot["x"], from_core, pl.ds(ROW_AT[c], SPANS[c])]

    def third(c, q, j):
        ga, gb, gf = SPLIT[c]
        off, flip = LINE[j]
        b_at = shifted(gb, (SIDE - TURNS[q]) % SIDE)
        return send(picked[c].at[q, j], landing(c, b_at, pos[gf], core), out_s.at[c, q], out_r.at[c, q], gf, off, flip)

    def stay(c, q):
        gb, gf = SPLIT[c][1:3]
        b_at = shifted(gb, (SIDE - TURNS[q]) % SIDE)
        return pltpu.make_async_copy(picked[c].at[q, len(LINE)], landing(c, b_at, pos[gf], core), local_sem.at[c, q])

    def bulk(ref, ssem, rsem):
        return send(ref, ref, ssem, rsem, "x", 0, 1)

    def all_asks():
        return bulk(rq, ask_s.at[0], ask_r.at[0])

    def all_onward(c):
        return bulk(gathered[c][3], fwd_s.at[c, 0], fwd_r.at[c])

    def all_third(c, q):
        return bulk(picked[c].at[q, pl.ds(0, len(LINE))], out_s.at[c, q], out_r.at[c, q])

    def mask_copy(g):
        rows = pl.ds(g * GROUP, GROUP)
        return pltpu.make_async_copy(mask_hbm.at[rows], masks.at[rows], mask_sem.at[g])

    def group_gives(g):
        rows = pl.ds(g * GROUP, GROUP)
        return (lambda: pltpu.make_async_copy(mb_ref.at[rows], mb_hbm.at[rows], mb_sem.at[g]),
                lambda: pltpu.make_async_copy(part_ref.at[rows], part_hbm.at[rows], part_sem.at[g]))

    for i in range(3):
        for c in EARLY:
            first(c, i).start()
    for i in range(len(PEER_LIST)):
        ask(i).start()
    for i in range(2):
        for c in EARLY:
            second(c, 0, i).start()
    for i in range(3):
        for c in LATER:
            first(c, i).start()
    for g in range(GROUPS):
        mask_copy(g).start()

    own_head = iota((HEADS, F), 1) // HD == iota((HEADS, F), 0)

    def spread(att):
        return jnp.where(own_head, jnp.concatenate([att] * HEADS, axis=1), 0.0)

    a_s = spread(atts_ref[...])
    a_d = spread(attd_ref[...])
    own = own_ref[...]
    a24 = stacked3(a_s)
    own_s = score_rows(a24, own)
    sig_col = jnp.max(own_s, axis=1, keepdims=True)
    sig_x = jnp.sum(jnp.where(own_head, sig_col, 0.0), axis=0, keepdims=True)
    par_ref[0:8] = a_s
    par_ref[8:16] = a_d
    par_ref[16:24] = jnp.broadcast_to(sig_col, (HEADS, F))
    par_ref[24:32] = jnp.broadcast_to(bias_ref[...], (8, F))
    own_low = jnp.broadcast_to(jnp.min(own_s - sig_col, axis=1, keepdims=True), (HEADS, F))

    same_head = iota((F, F), 0) // HD == iota((F, F), 1) // HD
    sx = nt_exact(own, jnp.where(same_head, jnp.sum(a_s, axis=0, keepdims=True), 0.0))
    dx = nt_exact(own, jnp.where(same_head, jnp.sum(a_d, axis=0, keepdims=True), 0.0))
    qx = jnp.exp(0.8 * jnp.minimum(dx + sig_x, LOW)).astype(BF)
    for h in range(HEADS // 2):
        wanted_row = (2 * h + iota((F, F), 1) // J) * HD
        pick_col = (iota((F, F), 0) == wanted_row).astype(F32).astype(BF)
        q_out[:, h] = jnp.dot(qx, pick_col, preferred_element_type=F32).astype(BF).reshape(NB, BLK, F)
    xo = sx - sig_x
    self_sums(acc_out, own, jnp.maximum(qx.astype(F32) * jnp.exp(xo), jnp.exp(0.2 * xo)))
    gives = [
        pltpu.make_async_copy(src, dst, give_sem.at[i])
        for i, (src, dst) in enumerate(((own_ref, own_hbm), (q_out, q_hbm), (acc_out, acc_hbm)))
    ]
    for g in gives:
        g.start()

    count = cnt_ref[0, 0]
    left = iota((BLK, BLK), 1) < J
    lane_marks(head_ref, ones_ref)

    def prepare(g, _):
        mask_copy(g).wait()
        for k in range(GROUP):
            t = g * GROUP + k
            m = masks[t].astype(F32) * (t < count).astype(F32)
            turned = pltpu.roll(m, J, 1)
            ma_ref[t] = jnp.where(left, m, turned).astype(BF)
            mb_ref[t] = jnp.where(left, turned, m).astype(BF)
        group_gives(g)[0]().start()
        return 0

    lax.fori_loop(0, GROUPS // 2, prepare, 0)

    def spread_second(ways):
        for k in range(1, SIDE):
            for c in ways:
                first(c, k - 1, True).wait_recv()
                for i in range(2):
                    second(c, k, i).start()

    spread_second(EARLY)
    all_asks().wait_recv()
    fetch = pltpu.make_async_copy(rq, rqs, smem_sem.at[0])
    fetch.start()
    fetch.wait()

    def pick(c, q):
        ga, gb, gf = SPLIT[c]
        b_at = shifted(gb, (SIDE - TURNS[q]) % SIDE)
        for j in range(len(LINE) + 1):
            for a_at in range(SIDE):
                col = place({ga: a_at, gb: b_at, gf: pos[gf]}, core)
                if j < len(LINE):
                    off, flip = LINE[j]
                    block = rqs[peer_slot(gf, (SIDE - off) % SIDE, flip), 0, col]
                else:
                    block = req_s[0, col]
                part = gathered[c][q][a_at, block]
                if c in EARLY and j == len(LINE):
                    spot = {ga: a_at, gb: b_at, gf: pos[gf]}
                    fara_ref[spot["y"], spot["z"], spot["x"], core, pl.ds(ROW_AT[c], SPANS[c])] = part
                else:
                    picked[c][q, j, a_at] = part

    def pass_on(c, q):
        for k in range(SIDE):
            second(c, k, q - 1).wait_recv()
            onward(c, k, q - 1).start()

    def hand_out(c, q):
        pick(c, q)
        for j in range(len(LINE)):
            third(c, q, j).start()
        if c in LATER:
            stay(c, q).start()

    for c in EARLY:
        hand_out(c, 0)
    lax.fori_loop(GROUPS // 2, GROUPS, prepare, 0)
    for i in range(2):
        for c in LATER:
            second(c, 0, i).start()
    spread_second(LATER)
    for q in (1, 2):
        for c in EARLY:
            pass_on(c, q)
            hand_out(c, q)
    for c in EARLY:
        all_onward(c).wait_recv()
        hand_out(c, 3)
    for q in (1, 2):
        for c in LATER:
            pass_on(c, q)
    for q in (0, 1, 2):
        for c in LATER:
            hand_out(c, q)
    for q in range(SIDE):
        for c in EARLY:
            all_third(c, q).wait_recv()

    def far_part(c, carry):
        p = c * PART
        return half_scores(fara_flat, a24, sig_col, b_ref, d_ref, p, PART, carry)

    fara_flat = fara_ref.reshape(PEERS, J, F)
    low, high = lax.fori_loop(0, PEERS // PART, far_part, (own_low, jnp.zeros((HEADS, F), F32)))
    par_ref[32:40] = low
    par_ref[40:48] = high
    last = (pltpu.make_async_copy(par_ref, par_hbm, give_sem.at[3]),
            pltpu.make_async_copy(fara_ref, fara_hbm, give_sem.at[4]))
    for copy in last:
        copy.start()

    def group(g, _):
        head_id = head_ref[...]
        for k in range(GROUP):
            src = src_ref[0, g * GROUP + k]
            v_ref[k] = fara_flat[src]
            factor_rows(k, src, b_ref, d_ref, bd_ref)
        for k in range(GROUP):
            t = g * GROUP + k
            sums = half_tile(k, dst_ref[0, t], q_out, v_ref[k], ma_ref[t], bd_ref, head_id, ones_ref)
            for side in range(2):
                part_ref[t, :, side * F:(side + 1) * F] = sums[side].astype(BF)
        group_gives(g)[1]().start()
        return 0

    for c in LATER:
        all_onward(c).wait_recv()
        hand_out(c, 3)

    lax.fori_loop(0, GROUPS, group, 0)

    for g in gives:
        g.wait()
    for copy in last:
        copy.wait()
    all_asks().wait_send()
    for c in range(WAYS):
        bulk(gathered[c][0].at[pl.ds(0, 3)], one_s.at[c], one_r.at[c, 0]).wait_send()
        for i in range(2):
            bulk(gathered[c][i + 1], two_s.at[c, i], two_r.at[c, 0, 0]).wait_send()
            bulk(gathered[c][3].at[:, pl.ds(0, NB // 2)], fwd_s.at[c, i], fwd_r.at[c]).wait_send()
    for g in range(GROUPS):
        for copy in group_gives(g):
            copy().wait()
    for q in range(SIDE):
        for c in range(WAYS):
            all_third(c, q).wait_send()
        for c in LATER:
            stay(c, q).wait()
    for q in range(SIDE):
        for c in LATER:
            all_third(c, q).wait_recv()


def exchange(x, weight, requests, att_src, att_dst, out_bias, dst, src, count, masks):
    hbm = pl.BlockSpec(memory_space=pltpu.HBM)
    dma = pltpu.SemaphoreType.DMA
    peers = len(PEER_LIST)
    lines = len(LINE)
    far = (SIDE, SIDE, SIDE, 2, J, F)
    return pl.pallas_call(
        exchange_kernel,
        out_shape=(
            jax.ShapeDtypeStruct(far, BF),
            jax.ShapeDtypeStruct(far, BF),
            jax.ShapeDtypeStruct((NB * BLK, F), BF),
            jax.ShapeDtypeStruct((NB, HEADS // 2, BLK, F), BF),
            jax.ShapeDtypeStruct((NB, BLK, 2 * F), F32),
            jax.ShapeDtypeStruct((48, F), F32),
            jax.ShapeDtypeStruct((TILES, BLK, BLK), BF),
            jax.ShapeDtypeStruct((TILES, BLK, 2 * F), BF),
        ),
        in_specs=[hbm] * 10,
        out_specs=(hbm,) * 8,
        scratch_shapes=(
            [pltpu.VMEM((SIDE, NB, span, F), BF) for span in SPANS for _ in range(SIDE)]
            + [pltpu.VMEM((SIDE, lines + 1, SIDE, span, F), BF) for span in SPANS]
            + [
                pltpu.VMEM((NB * BLK, F), BF),
                pltpu.VMEM((F, F), BF),
                pltpu.VMEM((1, PEERS), jnp.int32),
                pltpu.VMEM((HEADS, HD), F32),
                pltpu.VMEM((HEADS, HD), F32),
                pltpu.VMEM((1, F), F32),
                pltpu.SMEM((1, PEERS), jnp.int32),
                pltpu.VMEM((peers, 1, PEERS), jnp.int32),
                pltpu.SMEM((peers, 1, PEERS), jnp.int32),
                pltpu.VMEM((NB * BLK, F), BF),
                pltpu.VMEM((NB, BLK, 2 * F), F32),
                pltpu.VMEM((48, F), F32),
                pltpu.VMEM(far, BF),
                pltpu.VMEM((TILES, BLK, BLK), jnp.int32),
                pltpu.VMEM((PEERS, HEADS, BLK), F32),
                pltpu.VMEM((PEERS, HEADS, BLK), F32),
                pltpu.SMEM((1, TILES), jnp.int32),
                pltpu.SMEM((1, TILES), jnp.int32),
                pltpu.SMEM((1, 1), jnp.int32),
                dma((10,)), dma((5,)), dma((GROUPS,)), dma((GROUPS,)), dma((GROUPS,)),
                dma((1,)), dma((1,)),
                dma((WAYS,)), dma((WAYS, 3)),
                dma((WAYS, 2)), dma((WAYS, SIDE, 2)),
                dma((WAYS, 2)), dma((WAYS,)),
                dma((WAYS, SIDE)), dma((WAYS, SIDE)),
                dma((WAYS, SIDE)), dma((1,)),
            ]
        ),
        compiler_params=pltpu.CompilerParams(
            collective_id=0, has_side_effects=True, vmem_limit_bytes=VMEM_ALL
        ),
        name="exchange",
    )(x, weight, requests, att_src, att_dst, out_bias.reshape(1, F), dst, src, count, masks)


def local(node_feats, weight, att_src, att_dst, out_bias, requests, tile_dst, tile_src, tile_masks, tile_count):
    count = tile_count.reshape(1, 1)
    masks = tile_masks[0]
    fara, farb, *rest = exchange(node_feats, weight, requests, att_src, att_dst, out_bias, tile_dst, tile_src, count, masks)
    fara = fara.reshape(PEERS, J, F)
    farb = farb.reshape(PEERS, J, F)
    return attend(tile_dst, tile_src, count, fara, farb, *rest, masks)


def solution(mesh):
    placed = (
        P("node", None), P(), P(), P(), P(), P("node", None), P("node", None), P("node", None),
        P("node", None, None, None), P("node"),
    )
    return jax.shard_map(local, mesh=mesh, in_specs=placed, out_specs=P("node", None), check_vma=False)
```
